8 devices in a mesh: dp: 4 (over z, y, x), pp: 2 (over core).
Axes of the slice: x: 2, y: 2, z: 1, core: 2. Of those that a mesh axis runs over, the one named last changes fastest.
Arguments:
- tok_ids: int32 [2, 8, 130], P(None, 'dp')
- emb_s: bfloat16 [2, 92544, 2048], P('pp', 'dp')
- w_one: bfloat16 [2, 2, 2048, 8192], P('pp')
- w_two: bfloat16 [2, 2, 8192, 2048], P('pp')
- gain_f: bfloat16 [2048], replicated
- gain_h: bfloat16 [2048], replicated
- gain_e: bfloat16 [2048], replicated
- gain_m: bfloat16 [2048], replicated
- w_proj: bfloat16 [4096, 2048], replicated
- u_one: bfloat16 [2048, 8192], replicated
- u_two: bfloat16 [8192, 2048], replicated
- w_out: bfloat16 [2048, 92544], replicated
Outputs:
- output 1: float32 [], replicated
- output 2: float32 [2, 8, 128], P(None, 'dp')
- output 3: float32 [2, 8, 128], P(None, 'dp')
All inputs are finite; a program needn't handle non-finite values.
Results may differ from the reference program's by a relative error of at most 0.00260037.
Values are sent between devices in bfloat16 or wider.
A program may use at most 2.75 GiB of HBM per device.

```python
import jax
import jax.numpy as jnp
from jax import lax

STAGES = 2
LAYERS = 2
MICRO_BATCHES = 2
GLOBAL_BATCH = 8
SEQ_LEN = 128
HIDDEN = 2048
FFN_HIDDEN = 8192
VOCAB_SIZE = 92544
HEAD_ROWS = 128
NORM_EPS = 1e-6
MTP_WEIGHT = 0.3


def setup_inputs(seed: int = 0) -> dict:
    key_list = jax.random.split(jax.random.key(seed), 12)
    tok_ids = jax.random.randint(key_list[0], (MICRO_BATCHES, GLOBAL_BATCH, SEQ_LEN + 2), 0, VOCAB_SIZE, dtype=jnp.int32)
    tok_ids = tok_ids.at[0, 0, 0].set(0).at[0, 0, 1].set(VOCAB_SIZE - 1)
    table = jax.random.normal(key_list[1], (VOCAB_SIZE, HIDDEN), jnp.float32).astype(jnp.bfloat16)
    emb_s = jnp.concatenate([table[None], jnp.zeros((STAGES - 1, VOCAB_SIZE, HIDDEN), jnp.bfloat16)], axis=0)
    w_one = (jax.random.normal(key_list[2], (STAGES, LAYERS, HIDDEN, FFN_HIDDEN), jnp.float32) * HIDDEN ** -0.5).astype(jnp.bfloat16)
    w_two = (jax.random.normal(key_list[3], (STAGES, LAYERS, FFN_HIDDEN, HIDDEN), jnp.float32) * FFN_HIDDEN ** -0.5).astype(jnp.bfloat16)
    gain_f = jax.random.uniform(key_list[4], (HIDDEN,), jnp.float32, 0.25, 1.75).astype(jnp.bfloat16)
    gain_h = jax.random.uniform(key_list[5], (HIDDEN,), jnp.float32, 0.25, 1.75).astype(jnp.bfloat16)
    gain_e = jax.random.uniform(key_list[6], (HIDDEN,), jnp.float32, 0.25, 1.75).astype(jnp.bfloat16)
    gain_m = jax.random.uniform(key_list[7], (HIDDEN,), jnp.float32, 0.25, 1.75).astype(jnp.bfloat16)
    w_proj = (jax.random.normal(key_list[8], (2 * HIDDEN, HIDDEN), jnp.float32) * (2 * HIDDEN) ** -0.5).astype(jnp.bfloat16)
    u_one = (jax.random.normal(key_list[9], (HIDDEN, FFN_HIDDEN), jnp.float32) * HIDDEN ** -0.5).astype(jnp.bfloat16)
    u_two = (jax.random.normal(key_list[10], (FFN_HIDDEN, HIDDEN), jnp.float32) * FFN_HIDDEN ** -0.5).astype(jnp.bfloat16)
    w_out = (jax.random.normal(key_list[11], (HIDDEN, VOCAB_SIZE), jnp.float32) * 3.0 * HIDDEN ** -0.5).astype(jnp.bfloat16)
    return {'tok_ids': tok_ids, 'emb_s': emb_s, 'w_one': w_one, 'w_two': w_two, 'gain_f': gain_f, 'gain_h': gain_h, 'gain_e': gain_e, 'gain_m': gain_m, 'w_proj': w_proj, 'u_one': u_one, 'u_two': u_two, 'w_out': w_out}


def norm_plain(x_val):
    x_f = x_val.astype(jnp.float32)
    return (x_f * lax.rsqrt(jnp.mean(x_f * x_f, axis=-1, keepdims=True) + NORM_EPS)).astype(jnp.bfloat16)


def norm_gain(x_val, gain_vec):
    x_f = x_val.astype(jnp.float32)
    scaled = x_f * lax.rsqrt(jnp.mean(x_f * x_f, axis=-1, keepdims=True) + NORM_EPS)
    return (scaled * gain_vec.astype(jnp.float32)).astype(jnp.bfloat16)


def mlp_add(x_val, normed, w_up, w_down):
    hidden = jax.nn.gelu(jnp.dot(normed, w_up, preferred_element_type=jnp.float32)).astype(jnp.bfloat16)
    return (x_val.astype(jnp.float32) + jnp.dot(hidden, w_down, preferred_element_type=jnp.float32)).astype(jnp.bfloat16)


def row_nll(normed, targets, w_out):
    n_blocks = normed.shape[0] // HEAD_ROWS

    def one_block(pair):
        block_rows, block_tgt = pair
        logits = jnp.dot(block_rows, w_out, preferred_element_type=jnp.float32)
        picked = jnp.take_along_axis(logits, block_tgt[:, None], axis=1)[:, 0]
        return jax.nn.logsumexp(logits, axis=1) - picked

    per_block = lax.map(one_block, (normed.reshape(n_blocks, HEAD_ROWS, HIDDEN), targets.reshape(n_blocks, HEAD_ROWS)))
    return per_block.reshape(n_blocks * HEAD_ROWS)


def reference(tok_ids, emb_s, w_one, w_two, gain_f, gain_h, gain_e, gain_m, w_proj, u_one, u_two, w_out):
    table = emb_s[0]
    w_up = w_one.reshape(STAGES * LAYERS, HIDDEN, FFN_HIDDEN)
    w_down = w_two.reshape(STAGES * LAYERS, FFN_HIDDEN, HIDDEN)
    seqs = tok_ids.reshape(MICRO_BATCHES * GLOBAL_BATCH, SEQ_LEN + 2)

    def layer_step(x_val, weights):
        w_a, w_b = weights
        return mlp_add(x_val, norm_plain(x_val), w_a, w_b), None

    def per_sequence(ids):
        x_val = table[ids[:SEQ_LEN]]
        h_last, _ = lax.scan(layer_step, x_val, (w_up, w_down))
        main_nll = row_nll(norm_gain(h_last, gain_f), ids[1:SEQ_LEN + 1], w_out)
        e_rows = table[ids[1:SEQ_LEN + 1]]
        joined = jnp.concatenate([norm_gain(h_last, gain_h), norm_gain(e_rows, gain_e)], axis=1)
        z_val = jnp.dot(joined, w_proj, preferred_element_type=jnp.float32).astype(jnp.bfloat16)
        z_val = mlp_add(z_val, norm_gain(z_val, gain_m), u_one, u_two)
        mtp_nll = row_nll(norm_gain(z_val, gain_f), ids[2:], w_out)
        return main_nll, mtp_nll

    main_nll, mtp_nll = lax.map(per_sequence, seqs)
    main_nll = main_nll.reshape(MICRO_BATCHES, GLOBAL_BATCH, SEQ_LEN)
    mtp_nll = mtp_nll.reshape(MICRO_BATCHES, GLOBAL_BATCH, SEQ_LEN)
    total_loss = jnp.mean(main_nll) + MTP_WEIGHT * jnp.mean(mtp_nll)
    return (total_loss, main_nll, mtp_nll)
```

```python
import functools

import jax
import jax.numpy as jnp
from jax import lax
from jax.experimental import pallas as pl
from jax.experimental.pallas import tpu as pltpu
from jax.sharding import PartitionSpec as P

NORM_EPS = 1e-6
MTP_WEIGHT = 0.3
F32 = jnp.float32
BF16 = jnp.bfloat16
VMEM_BYTES = 60 * 1024 * 1024

ROWS_A = 288
FFN_TILE = 1024
HEAD_HALF = 1024
CAP_A = 104
CAP_B = 88


def rms(x_f):
    return x_f * lax.rsqrt(jnp.mean(x_f * x_f, axis=-1, keepdims=True) + NORM_EPS)


def rms_gain(x_val, gain_ref):
    return (rms(x_val.astype(F32)) * gain_ref[...].astype(F32)).astype(BF16)


def dot32(a, b):
    return jnp.dot(a, b, preferred_element_type=F32)


def ffn_steps(j, n_tiles, n_s, w1_ref, w2_ref, h0, h1, acc, finish):
    def up(h_ref):
        h_ref[...] = jax.nn.gelu(dot32(n_s[...], w1_ref[...])).astype(BF16)

    def down(h_ref):
        acc[...] += dot32(h_ref[...], w2_ref[...])

    @pl.when(j == 0)
    def _():
        up(h0)

    @pl.when((j > 0) & (j < n_tiles) & (j % 2 == 1))
    def _():
        up(h1)
        down(h0)

    @pl.when((j > 0) & (j < n_tiles) & (j % 2 == 0))
    def _():
        up(h0)
        down(h1)

    @pl.when(j == n_tiles)
    def _():
        last = h1 if n_tiles % 2 == 0 else h0
        finish(dot32(last[...], w2_ref[...]))


def layers_kernel(n_tiles, x_ref, w1_ref, w2_ref, o_ref, x_s, n_s, h0, h1, acc):
    layer, j = pl.program_id(0), pl.program_id(1)

    @pl.when((layer == 0) & (j == 0))
    def _():
        x_s[...] = x_ref[...]

    @pl.when(j == 0)
    def _():
        n_s[...] = rms(x_s[...].astype(F32)).astype(BF16)
        acc[...] = jnp.zeros_like(acc)

    def finish(last):
        out = (x_s[...].astype(F32) + (acc[...] + last)).astype(BF16)
        x_s[...] = out
        o_ref[...] = out

    ffn_steps(j, n_tiles, n_s, w1_ref, w2_ref, h0, h1, acc, finish)


def run_layers(x_val, w_one, w_two):
    rows, width = x_val.shape
    _, n_layers, _, ffn = w_one.shape
    n_tiles = ffn // FFN_TILE
    whole = pl.BlockSpec((rows, width), lambda l, j: (0, 0))
    return pl.pallas_call(
        functools.partial(layers_kernel, n_tiles),
        out_shape=jax.ShapeDtypeStruct((rows, width), BF16),
        grid=(n_layers, n_tiles + 1),
        in_specs=[
            whole,
            pl.BlockSpec((None, None, width, FFN_TILE), lambda l, j: (0, l, 0, jnp.minimum(j, n_tiles - 1))),
            pl.BlockSpec((None, None, FFN_TILE, width), lambda l, j: (0, l, jnp.maximum(j - 1, 0), 0)),
        ],
        out_specs=whole,
        scratch_shapes=[
            pltpu.VMEM((rows, width), BF16),
            pltpu.VMEM((rows, width), BF16),
            pltpu.VMEM((rows, FFN_TILE), BF16),
            pltpu.VMEM((rows, FFN_TILE), BF16),
            pltpu.VMEM((rows, width), F32),
        ],
        compiler_params=pltpu.CompilerParams(dimension_semantics=("arbitrary", "arbitrary"), vmem_limit_bytes=VMEM_BYTES),
        cost_estimate=pl.CostEstimate(
            flops=4 * rows * width * ffn * n_layers, bytes_accessed=4 * width * ffn * n_layers, transcendentals=0
        ),
        name="layers",
    )(x_val, w_one, w_two)


def mtp_kernel(
    n_proj, n_tiles, h_ref, e_ref, gf_ref, gh_ref, ge_ref, gm_ref, wp_ref, w1_ref, w2_ref, o_ref,
    cat_s, z_s, n_s, h0, h1, acc,
):
    step = pl.program_id(0)
    rows, width = h_ref.shape
    proj_tile = wp_ref.shape[0]

    @pl.when(step == 0)
    def _():
        cat_s[:, :width] = rms_gain(h_ref[...], gh_ref)
        cat_s[:, width:] = rms_gain(e_ref[...], ge_ref)
        o_ref[:rows, :] = rms_gain(h_ref[...], gf_ref)
        acc[...] = jnp.zeros_like(acc)

    for k in range(n_proj):
        @pl.when(step == k)
        def _():
            acc[...] += dot32(cat_s[:, k * proj_tile:(k + 1) * proj_tile], wp_ref[...])

    @pl.when(step == n_proj - 1)
    def _():
        z_s[...] = acc[...].astype(BF16)
        n_s[...] = rms_gain(z_s[...], gm_ref)
        acc[...] = jnp.zeros_like(acc)

    def finish(last):
        z_new = (z_s[...].astype(F32) + (acc[...] + last)).astype(BF16)
        o_ref[rows:, :] = rms_gain(z_new, gf_ref)

    ffn_steps(step - n_proj, n_tiles, n_s, w1_ref, w2_ref, h0, h1, acc, finish)


def run_mtp(h_last, e_rows, gain_f, gain_h, gain_e, gain_m, w_proj, u_one, u_two):
    rows, width = h_last.shape
    ffn = u_one.shape[1]
    n_tiles = ffn // FFN_TILE
    n_proj = w_proj.shape[0] // FFN_TILE
    whole = pl.BlockSpec((rows, width), lambda s: (0, 0))
    gain = pl.BlockSpec((1, width), lambda s: (0, 0))
    return pl.pallas_call(
        functools.partial(mtp_kernel, n_proj, n_tiles),
        out_shape=jax.ShapeDtypeStruct((2 * rows, width), BF16),
        grid=(n_proj + n_tiles + 1,),
        in_specs=[
            whole, whole, gain, gain, gain, gain,
            pl.BlockSpec((FFN_TILE, width), lambda s: (jnp.minimum(s, n_proj - 1), 0)),
            pl.BlockSpec((width, FFN_TILE), lambda s: (0, jnp.clip(s - n_proj, 0, n_tiles - 1))),
            pl.BlockSpec((FFN_TILE, width), lambda s: (jnp.clip(s - n_proj - 1, 0, n_tiles - 1), 0)),
        ],
        out_specs=pl.BlockSpec((2 * rows, width), lambda s: (0, 0)),
        scratch_shapes=[
            pltpu.VMEM((rows, 2 * width), BF16),
            pltpu.VMEM((rows, width), BF16),
            pltpu.VMEM((rows, width), BF16),
            pltpu.VMEM((rows, FFN_TILE), BF16),
            pltpu.VMEM((rows, FFN_TILE), BF16),
            pltpu.VMEM((rows, width), F32),
        ],
        compiler_params=pltpu.CompilerParams(dimension_semantics=("arbitrary",), vmem_limit_bytes=VMEM_BYTES),
        cost_estimate=pl.CostEstimate(
            flops=4 * rows * width * (ffn + width), bytes_accessed=4 * width * (ffn + width), transcendentals=0
        ),
        name="mtp",
    )(h_last, e_rows, gain_f[None], gain_h[None], gain_e[None], gain_m[None], w_proj, u_one, u_two)


LANES = 128
GROUP = 16


def head_stats(buf, n_cols, base, tgt_ref, m_ref, s_ref, p_ref):
    rows = buf.shape[0]
    lane = lax.broadcasted_iota(jnp.int32, (GROUP, LANES), 1)
    for r in range(0, rows, GROUP):
        rs = slice(r, r + GROUP)
        parts = [buf[rs, c:c + LANES] for c in range(0, n_cols, LANES)]
        top = parts[0]
        for part in parts[1:]:
            top = jnp.maximum(top, part)
        m_old = m_ref[rs, :]
        m_new = jnp.maximum(m_old, top)
        total = s_ref[rs, :] * jnp.exp(m_old - m_new)
        rel = tgt_ref[rs, :] - lane - base
        pick = p_ref[rs, :]
        for k, part in enumerate(parts):
            total = total + jnp.exp(part - m_new)
            pick = jnp.where(rel == k * LANES, part, pick)
        m_ref[rs, :] = m_new
        s_ref[rs, :] = total
        p_ref[rs, :] = pick


def head_kernel(n_steps, tail, x_ref, tgt_ref, w_ref, o_ref, buf_a, buf_b, m_ref, s_ref, p_ref):
    i = pl.program_id(0)
    half = buf_a.shape[1]
    state = (tgt_ref, m_ref, s_ref, p_ref)

    @pl.when(i == 0)
    def _():
        buf_b[...] = jnp.full_like(buf_b, -3e38)
        m_ref[...] = jnp.full_like(m_ref, -3e38)
        s_ref[...] = jnp.zeros_like(s_ref)
        p_ref[...] = jnp.zeros_like(p_ref)

    @pl.when(i < n_steps - 1)
    def _():
        buf_a[...] = dot32(x_ref[...], w_ref[:, :half])
        head_stats(buf_b, half, (2 * i - 1) * half, *state)
        buf_b[...] = dot32(x_ref[...], w_ref[:, half:])
        head_stats(buf_a, half, 2 * i * half, *state)

    @pl.when(i == n_steps - 1)
    def _():
        head_stats(buf_b, half, (2 * i - 1) * half, *state)
        done = 0
        while done < tail:
            cols = min(half, tail - done)
            buf_a[:, :cols] = dot32(x_ref[...], w_ref[:, done:done + cols])
            head_stats(buf_a, cols, 2 * i * half + done, *state)
            done += cols
        top = jnp.max(m_ref[...], axis=1, keepdims=True)
        total = jnp.sum(s_ref[...] * jnp.exp(m_ref[...] - top), axis=1, keepdims=True)
        picked = jnp.sum(p_ref[...], axis=1, keepdims=True)
        o_ref[...] = jnp.broadcast_to(top + jnp.log(total) - picked, o_ref.shape)


def run_head(x_val, targets, w_out):
    rows, width = x_val.shape
    vocab = w_out.shape[1]
    tile = 2 * HEAD_HALF
    n_steps = pl.cdiv(vocab, tile)
    tail = vocab - (n_steps - 1) * tile
    out = pl.pallas_call(
        functools.partial(head_kernel, n_steps, tail),
        out_shape=jax.ShapeDtypeStruct((rows, LANES), F32),
        grid=(n_steps,),
        in_specs=[
            pl.BlockSpec((rows, width), lambda i: (0, 0)),
            pl.BlockSpec((rows, LANES), lambda i: (0, 0)),
            pl.BlockSpec((width, tile), lambda i: (0, i)),
        ],
        out_specs=pl.BlockSpec((rows, LANES), lambda i: (0, 0)),
        scratch_shapes=[
            pltpu.VMEM((rows, HEAD_HALF), F32),
            pltpu.VMEM((rows, HEAD_HALF), F32),
            pltpu.VMEM((rows, LANES), F32),
            pltpu.VMEM((rows, LANES), F32),
            pltpu.VMEM((rows, LANES), F32),
        ],
        compiler_params=pltpu.CompilerParams(dimension_semantics=("arbitrary",), vmem_limit_bytes=VMEM_BYTES),
        cost_estimate=pl.CostEstimate(flops=2 * rows * width * vocab, bytes_accessed=2 * width * vocab, transcendentals=0),
        name="head",
    )(x_val, jnp.broadcast_to(targets[:, None], (rows, LANES)), w_out)
    return out[:, 0]


def solution(mesh):
    n_data = mesh.shape["dp"]
    n_stages = mesh.shape["pp"]

    def flat(dp_idx, pp_idx):
        return dp_idx * n_stages + pp_idx

    def swap_perm(k):
        return [(flat(d, 0), flat(d ^ k, 0)) for d in range(n_data)]

    def fetch_rows(table, ids_all, cap):
        me = lax.axis_index("dp")
        n_local = table.shape[0]
        n = ids_all.shape[1]
        owner = ids_all // n_local
        same = owner[:, :, None] == jnp.arange(n_data)[None, None, :]
        most = jnp.max(jnp.sum(same.astype(jnp.int32), axis=1))
        before = jnp.arange(n)[:, None] < jnp.arange(n)[None, :]
        rank_all = jnp.einsum(
            "dns,nm->dms", same.astype(BF16), before.astype(BF16), preferred_element_type=F32
        ).astype(jnp.int32)
        dests = jnp.bitwise_xor(me, jnp.arange(n_data))
        mine = jnp.take(same, me, axis=2)[dests]
        my_rank = jnp.take(rank_all, me, axis=2)[dests]
        local = (ids_all - me * n_local)[dests]
        own_src = jnp.bitwise_xor(owner[me], me)
        own_rank = jnp.sum(jnp.where(same[me], rank_all[me], 0), axis=1)

        def one_round(j):
            slot = j * cap + jnp.arange(cap)
            hit = mine[:, None, :] & (my_rank[:, None, :] == slot[None, :, None])
            idx = jnp.sum(jnp.where(hit, local[:, None, :], 0), axis=2)
            packed = [table[idx[k]] for k in range(n_data)]
            got = [packed[0]] + [lax.ppermute(packed[k], ("dp", "pp"), swap_perm(k)) for k in range(1, n_data)]
            in_round = (own_rank >= j * cap) & (own_rank < (j + 1) * cap)
            place = jnp.where(in_round, own_src * cap + own_rank - j * cap, -1)
            pick = (place[:, None] == jnp.arange(n_data * cap)[None, :]).astype(BF16)
            return dot32(pick, jnp.concatenate(got, axis=0)).astype(BF16)

        first = one_round(0)
        _, rows = lax.while_loop(
            lambda c: c[0] * cap < most, lambda c: (c[0] + 1, c[1] + one_round(c[0])), (jnp.int32(1), first)
        )
        return rows

    def body(tok_ids, emb_s, w_one, w_two, gain_f, gain_h, gain_e, gain_m, w_proj, u_one, u_two, w_out):
        stage = lax.axis_index("pp")
        n_micro, batch_dev, seq_plus = tok_ids.shape
        seq_len = seq_plus - 2
        n_seq = n_micro * batch_dev
        n_tok = n_seq * seq_len
        rows_a = ROWS_A
        rows_b = n_tok - rows_a
        table = emb_s[0]
        ids = tok_ids.reshape(n_seq, seq_plus)
        want = ids[:, :seq_len + 1].reshape(n_seq * (seq_len + 1))
        ids_all = lax.all_gather(want, "dp")
        cut = rows_a + (rows_a - 1) // seq_len

        rows_lo = fetch_rows(table, ids_all[:, :cut], CAP_A)
        rows_hi = fetch_rows(table, ids_all[:, cut:], CAP_B)

        def tokens(rows, shift):
            return rows.reshape(n_seq, seq_len + 1, -1)[:, shift:shift + seq_len].reshape(n_tok, -1)

        lo_idx = [t + t // seq_len for t in range(rows_a)]
        x_a = jnp.concatenate(
            [rows_lo[s * (seq_len + 1):min(s * (seq_len + 1) + seq_len, cut)] for s in range(n_seq) if s * (seq_len + 1) < cut],
            axis=0,
        )
        assert x_a.shape[0] == len(lo_idx)
        x_a = run_layers(x_a, w_one, w_two)

        all_rows = jnp.concatenate([rows_lo, rows_hi], axis=0)
        x_b = jnp.pad(tokens(all_rows, 0)[rows_a:], ((0, rows_a - rows_b), (0, 0)))
        moved = lax.ppermute(x_a, "pp", [(0, 1)])
        e_all = lax.ppermute(all_rows, "pp", [(0, 1)])
        x_mid = run_layers(jnp.where(stage == 0, x_b, moved), w_one, w_two)
        swapped = lax.ppermute(x_mid, "pp", [(0, 1), (1, 0)])
        e_rows = tokens(jnp.where(stage == 0, all_rows, e_all), 1)
        tgt_main = ids[:, 1:seq_len + 1].reshape(n_tok)
        tgt_mtp = ids[:, 2:].reshape(n_tok)

        def tail(h_last, lo, hi):
            rows = run_mtp(h_last, e_rows[lo:hi], gain_f, gain_h, gain_e, gain_m, w_proj, u_one, u_two)
            nll = run_head(rows, jnp.concatenate([tgt_main[lo:hi], tgt_mtp[lo:hi]]), w_out)
            pad = lambda v: jnp.pad(v, (lo, n_tok - hi))
            return pad(nll[:hi - lo]), pad(nll[hi - lo:])

        def tail_first(swapped):
            return tail(swapped, 0, rows_a)

        def tail_last(swapped):
            return tail(run_layers(swapped[:rows_b], w_one, w_two), rows_a, n_tok)

        main_part, mtp_part = lax.cond(stage == 0, tail_first, tail_last, swapped)
        local_sum = jnp.sum(main_part) + MTP_WEIGHT * jnp.sum(mtp_part)
        main_nll = lax.psum(main_part, "pp").reshape(n_micro, batch_dev, seq_len)
        mtp_nll = lax.psum(mtp_part, "pp").reshape(n_micro, batch_dev, seq_len)
        total_loss = lax.psum(local_sum, ("dp", "pp")) / (n_tok * n_data)
        return total_loss, main_nll, mtp_nll

    rep = P()
    in_specs = (P(None, "dp", None), P("pp", "dp", None), P("pp"), P("pp")) + (rep,) * 8
    out_specs = (rep, P(None, "dp", None), P(None, "dp", None))
    return jax.shard_map(body, mesh=mesh, in_specs=in_specs, out_specs=out_specs, check_vma=False)
```

```python
import functools

import jax
import jax.numpy as jnp
from jax import lax
from jax.experimental import pallas as pl
from jax.experimental.pallas import tpu as pltpu
from jax.sharding import PartitionSpec as P

NORM_EPS = 1e-6
MTP_WEIGHT = 0.3
F32 = jnp.float32
BF16 = jnp.bfloat16
I32 = jnp.int32
MESH = pl.DeviceIdType.MESH
VMEM_BYTES = 60 * 1024 * 1024
LANES = 128
GROUP = 16

ROWS_A = 288
FFN_TILE = 1024
HEAD_HALF = 1024
CAP = 176
BLOCK = 8


def rms(x_f):
    return x_f * lax.rsqrt(jnp.mean(x_f * x_f, axis=-1, keepdims=True) + NORM_EPS)


def rms_gain(x_val, gain_ref):
    return (rms(x_val.astype(F32)) * gain_ref[...].astype(F32)).astype(BF16)


def dot32(a, b):
    return jnp.dot(a, b, preferred_element_type=F32)


def norm_rows(dst, src, gain_ref=None, base=0):
    for r in range(0, src.shape[0], GROUP):
        val = rms(src[r:r + GROUP, :].astype(F32))
        if gain_ref is not None:
            val = val * gain_ref[...].astype(F32)
        dst[base + r:base + r + GROUP, :] = val.astype(BF16)


def collective(idx):
    return pltpu.CompilerParams(collective_id=idx, has_side_effects=True, vmem_limit_bytes=VMEM_BYTES)


def enter(peers):
    barrier = pltpu.get_barrier_semaphore()
    for peer in peers:
        pl.semaphore_signal(barrier, inc=1, device_id=peer, device_id_type=MESH)
    pl.semaphore_wait(barrier, len(peers))


def push(src, dst, send_sem, recv_sem, peer):
    return pltpu.make_async_remote_copy(
        src_ref=src, dst_ref=dst, send_sem=send_sem, recv_sem=recv_sem, device_id=peer, device_id_type=MESH
    )


def slot_ranks(held):
    row = lax.broadcasted_iota(I32, (LANES, LANES), 0)
    col = lax.broadcasted_iota(I32, (LANES, LANES), 1)
    ahead = dot32(held.astype(BF16), (row < col).astype(BF16))
    total = dot32(held.astype(BF16), jnp.ones((LANES, LANES), BF16))
    out, base = [], jnp.zeros((1, LANES), F32)
    for r in range(held.shape[0]):
        out.append(ahead[r:r + 1, :] + base)
        base = base + total[r:r + 1, :]
    return jnp.concatenate(out, axis=0)


def slots_kernel(n_data, n_local, ids_ref, idx_ref, most_ref, got, send_sem, recv_sem):
    me, stage = lax.axis_index("dp"), lax.axis_index("pp")
    peers = [(jnp.bitwise_xor(me, k), stage) for k in range(1, n_data)]
    enter(peers)
    copies = [push(ids_ref, got.at[k], send_sem.at[k], recv_sem.at[k], peer) for k, peer in enumerate(peers)]
    for copy in copies:
        copy.start()
    for copy in copies:
        copy.wait()
    most = jnp.zeros((1, 1), F32)
    slot = lax.broadcasted_iota(I32, (CAP, LANES), 0).astype(F32)
    for k in range(n_data):
        ids = ids_ref[...] if k == 0 else got[k - 1]
        for s in range(n_data):
            inside = ((ids >= s * n_local) & (ids < (s + 1) * n_local)).astype(F32)
            most = jnp.maximum(most, jnp.sum(jnp.sum(inside, axis=1, keepdims=True), axis=0, keepdims=True))
        local = ids - me * n_local
        held = ((local >= 0) & (local < n_local)).astype(F32)
        rank = jnp.where(held > 0, slot_ranks(held), -1.0)
        high = lax.shift_right_arithmetic(local, 8)
        low = (local - high * 256).astype(F32)
        high = high.astype(F32)
        acc = jnp.zeros((BLOCK, CAP), F32)
        for r in range(ids.shape[0]):
            hit = (jnp.broadcast_to(rank[r:r + 1, :], (CAP, LANES)) == slot).astype(BF16)
            keep = held[r:r + 1, :]
            pair = jnp.concatenate(
                [high[r:r + 1, :] * keep, low[r:r + 1, :] * keep, jnp.zeros((BLOCK - 2, LANES), F32)], axis=0
            ).astype(BF16)
            acc = acc + lax.dot_general(pair, hit, (((1,), (1,)), ((), ())), preferred_element_type=F32)
        idx_ref[k:k + 1, :CAP] = (acc[0:1, :] * 256.0 + acc[1:2, :]).astype(I32)
    most_ref[...] = jnp.broadcast_to(most, most_ref.shape).astype(I32)


def run_slots(ids_tile, n_data, n_local):
    vmem = pl.BlockSpec(memory_space=pltpu.VMEM)
    return pl.pallas_call(
        functools.partial(slots_kernel, n_data, n_local),
        out_shape=[jax.ShapeDtypeStruct((n_data, 2 * LANES), I32), jax.ShapeDtypeStruct((BLOCK, LANES), I32)],
        in_specs=[vmem],
        out_specs=[vmem, vmem],
        scratch_shapes=[
            pltpu.VMEM((n_data - 1, BLOCK, LANES), I32),
            pltpu.SemaphoreType.DMA((n_data - 1,)),
            pltpu.SemaphoreType.DMA((n_data - 1,)),
        ],
        compiler_params=collective(0),
        name="slots",
    )(ids_tile)


def pack_kernel(n_data, idx_ref, lane_ref, table_ref, o_ref, held, sems):
    parts = [(0, LANES), (LANES, CAP - LANES)]

    @pl.when(lax.axis_index("pp") == 0)
    def _():
        for k in range(n_data):
            for p, (first, count) in enumerate(parts):
                def fetch(c, carry):
                    start = pl.multiple_of(lax.shift_right_logical(idx_ref[k, first + c], 3) * BLOCK, BLOCK)
                    to = pl.multiple_of((k * CAP + first + c) * BLOCK, BLOCK)
                    pltpu.make_async_copy(
                        table_ref.at[pl.ds(start, BLOCK), :], held.at[pl.ds(to, BLOCK), :], sems.at[k * 2 + p]
                    ).start()
                    return carry

                lax.fori_loop(0, count, fetch, 0, unroll=8)
        for k in range(n_data):
            for p, (first, count) in enumerate(parts):
                at = (k * CAP + first) * BLOCK
                span = count * BLOCK
                pltpu.make_async_copy(table_ref.at[pl.ds(0, span), :], held.at[pl.ds(at, span), :], sems.at[k * 2 + p]).wait()
                idx = jnp.broadcast_to(lane_ref[k:k + 1, p * LANES:(p + 1) * LANES].astype(F32), (LANES, LANES))
                idx = jnp.transpose(idx)[:count, :].astype(I32)
                low = jnp.bitwise_and(idx, BLOCK - 1)
                row = lax.broadcasted_iota(I32, (count, LANES), 0)
                lane = lax.broadcasted_iota(I32, (count, LANES), 1)
                picks = []
                for c in range(0, span, LANES):
                    at_row = c // BLOCK + lax.shift_right_logical(lane, 3)
                    picks.append(((row == at_row) & (low == jnp.bitwise_and(lane, BLOCK - 1))).astype(F32).astype(BF16))
                pick = jnp.concatenate(picks, axis=1)
                o_ref[k, first:first + count, :] = dot32(pick, held[at:at + span, :]).astype(BF16)


def run_pack(idx, table):
    n_data = idx.shape[0]
    width = table.shape[1]
    return pl.pallas_call(
        functools.partial(pack_kernel, n_data),
        out_shape=jax.ShapeDtypeStruct((n_data, CAP, width), BF16),
        in_specs=[
            pl.BlockSpec(memory_space=pltpu.SMEM),
            pl.BlockSpec(memory_space=pltpu.VMEM),
            pl.BlockSpec(memory_space=pl.ANY),
        ],
        out_specs=pl.BlockSpec(memory_space=pltpu.VMEM),
        scratch_shapes=[pltpu.VMEM((n_data * CAP * BLOCK, width), BF16), pltpu.SemaphoreType.DMA((2 * n_data,))],
        compiler_params=pltpu.CompilerParams(vmem_limit_bytes=VMEM_BYTES),
        name="pack",
    )(idx, idx, table)


def trade_kernel(n_data, n_local, n_seq, ids_ref, packed_ref, x_ref, e_ref, got, pick_s, send_sem, recv_sem):
    me, stage = lax.axis_index("dp"), lax.axis_index("pp")
    n_tok = n_seq * LANES
    if x_ref.shape[0] > n_tok:
        x_ref[n_tok:, :] = jnp.zeros((x_ref.shape[0] - n_tok, x_ref.shape[1]), BF16)

    @pl.when(stage == 0)
    def _():
        peers = [(jnp.bitwise_xor(me, k), stage) for k in range(1, n_data)]
        enter(peers)
        copies = [
            push(packed_ref.at[k + 1], got.at[k], send_sem.at[k], recv_sem.at[k], peer) for k, peer in enumerate(peers)
        ]
        for k in (2, 0, 1):
            copies[k].start()
        ids = ids_ref[...]
        slot = lax.broadcasted_iota(I32, (CAP, LANES), 0).astype(F32)
        lane = lax.broadcasted_iota(I32, (1, LANES), 1)
        for k in range(n_data):
            src = jnp.bitwise_xor(me, k)
            held = ((ids >= src * n_local) & (ids < (src + 1) * n_local)).astype(F32)
            rank = jnp.where(held > 0, slot_ranks(held), -1.0)
            ahead = pltpu.roll(rank, LANES - 1, 1)
            for s in range(n_seq):
                now = rank[2 * s:2 * s + 1, :]
                later = jnp.where(lane == LANES - 1, ahead[2 * s + 1:2 * s + 2, :], ahead[2 * s:2 * s + 1, :])
                for q, want in ((s, now), (n_seq + s, later)):
                    hit = (jnp.broadcast_to(want, (CAP, LANES)) == slot).astype(F32).astype(BF16)
                    pick_s[k * CAP:(k + 1) * CAP, q * LANES:(q + 1) * LANES] = hit

        def placed(k, block):
            return lax.dot_general(
                pick_s[k * CAP:(k + 1) * CAP, :], block, (((0,), (0,)), ((), ())), preferred_element_type=F32
            ).astype(BF16)

        def add(val):
            x_ref[:n_tok, :] += val[:n_tok]
            e_ref[:n_tok, :] += val[n_tok:]

        first = placed(0, packed_ref[0])
        x_ref[:n_tok, :] = first[:n_tok]
        e_ref[:n_tok, :] = first[n_tok:]
        for k in range(n_data - 1):
            copies[k].wait()
            add(placed(k + 1, got[k]))

    @pl.when(stage != 0)
    def _():
        x_ref[:n_tok, :] = jnp.zeros((n_tok, x_ref.shape[1]), BF16)
        e_ref[:n_tok, :] = jnp.zeros((n_tok, x_ref.shape[1]), BF16)


def run_trade(ids_tile, packed, n_local, n_seq, pad_rows):
    n_data, _, width = packed.shape
    n_tok = n_seq * LANES
    vmem = pl.BlockSpec(memory_space=pltpu.VMEM)
    return pl.pallas_call(
        functools.partial(trade_kernel, n_data, n_local, n_seq),
        out_shape=[jax.ShapeDtypeStruct((pad_rows, width), BF16), jax.ShapeDtypeStruct((n_tok, width), BF16)],
        in_specs=[vmem, vmem],
        out_specs=[vmem, vmem],
        scratch_shapes=[
            pltpu.VMEM((n_data - 1, CAP, width), BF16),
            pltpu.VMEM((n_data * CAP, 2 * n_tok), BF16),
            pltpu.SemaphoreType.DMA((n_data - 1,)),
            pltpu.SemaphoreType.DMA((n_data - 1,)),
        ],
        compiler_params=collective(1),
        name="trade",
    )(ids_tile, packed)


def hand_on_kernel(rows_a, x_ref, e_ref, x_out, e_out, send_sem, recv_sem):
    me, stage = lax.axis_index("dp"), lax.axis_index("pp")
    peer = (me, 1 - stage)
    enter([peer])
    copies = [
        push(x_ref, x_out, send_sem.at[0], recv_sem.at[0], peer),
        push(e_ref.at[pl.ds(rows_a, e_out.shape[0]), :], e_out, send_sem.at[1], recv_sem.at[1], peer),
    ]

    @pl.when(stage == 0)
    def _():
        for copy in copies:
            copy.start()
        for copy in copies:
            copy.wait_send()

    @pl.when(stage != 0)
    def _():
        for copy in copies:
            copy.wait_recv()


def run_hand_on(x_val, e_val):
    rows_a, width = x_val.shape
    rows_b = e_val.shape[0] - rows_a
    hbm = pl.BlockSpec(memory_space=pl.ANY)
    return pl.pallas_call(
        functools.partial(hand_on_kernel, rows_a),
        out_shape=[jax.ShapeDtypeStruct((rows_a, width), BF16), jax.ShapeDtypeStruct((rows_b, width), BF16)],
        in_specs=[hbm, hbm],
        out_specs=[hbm, hbm],
        scratch_shapes=[pltpu.SemaphoreType.DMA((2,)), pltpu.SemaphoreType.DMA((2,))],
        compiler_params=collective(2),
        name="hand_on",
    )(x_val, e_val)


def swap_kernel(x_ref, o_ref, send_sem, recv_sem):
    peer = (lax.axis_index("dp"), 1 - lax.axis_index("pp"))
    enter([peer])
    copy = push(x_ref, o_ref, send_sem, recv_sem, peer)
    copy.start()
    copy.wait()


def run_swap(x_val):
    hbm = pl.BlockSpec(memory_space=pl.ANY)
    return pl.pallas_call(
        swap_kernel,
        out_shape=jax.ShapeDtypeStruct(x_val.shape, BF16),
        in_specs=[hbm],
        out_specs=hbm,
        scratch_shapes=[pltpu.SemaphoreType.DMA, pltpu.SemaphoreType.DMA],
        compiler_params=collective(3),
        name="swap",
    )(x_val)


def finish_kernel(n_data, n_stages, scale, x_ref, nll_ref, total_ref, got, send_sem, recv_sem):
    me, stage = lax.axis_index("dp"), lax.axis_index("pp")
    mine = me * n_stages + stage
    steps = [(k, c) for k in range(n_data) for c in range(n_stages) if (k, c) != (0, 0)]
    peers = [(jnp.bitwise_xor(me, k), jnp.bitwise_xor(stage, c)) for k, c in steps]
    enter(peers)
    copies = [push(x_ref, got.at[mine], send_sem.at[i], recv_sem.at[i], peer) for i, peer in enumerate(peers)]
    for copy in copies:
        copy.start()
    for copy in copies:
        copy.wait()
    got[mine] = x_ref[...]
    half = x_ref.shape[0] // 2
    total = jnp.zeros(x_ref.shape, F32)
    for i in range(n_data * n_stages):
        total = total + got[i]
    main = jnp.sum(jnp.sum(total[:half], axis=1, keepdims=True), axis=0, keepdims=True)
    mtp = jnp.sum(jnp.sum(total[half:], axis=1, keepdims=True), axis=0, keepdims=True)
    total_ref[...] = jnp.broadcast_to((main + MTP_WEIGHT * mtp) * scale, total_ref.shape)
    nll = x_ref[...]
    for c in range(1, n_stages):
        nll = nll + got[me * n_stages + jnp.bitwise_xor(stage, c)]
    nll_ref[...] = nll


def run_finish(tile, n_data, n_stages, scale):
    vmem = pl.BlockSpec(memory_space=pltpu.VMEM)
    n_peers = n_data * n_stages - 1
    return pl.pallas_call(
        functools.partial(finish_kernel, n_data, n_stages, scale),
        out_shape=[jax.ShapeDtypeStruct(tile.shape, F32), jax.ShapeDtypeStruct(tile.shape, F32)],
        in_specs=[vmem],
        out_specs=[vmem, vmem],
        scratch_shapes=[
            pltpu.VMEM((n_data * n_stages,) + tile.shape, F32),
            pltpu.SemaphoreType.DMA((n_peers,)),
            pltpu.SemaphoreType.DMA((n_peers,)),
        ],
        compiler_params=collective(4),
        name="finish",
    )(tile)


def ffn_steps(j, n_tiles, n_s, w1_ref, w2_ref, raw, hid, acc, finish):
    def activate():
        for r in range(0, raw.shape[0], GROUP):
            for c in range(0, raw.shape[1], 2 * LANES):
                spot = (slice(r, r + GROUP), slice(c, c + 2 * LANES))
                hid[spot] = jax.nn.gelu(raw[spot]).astype(BF16)

    @pl.when(j == 0)
    def _():
        raw[...] = dot32(n_s[...], w1_ref[...])

    @pl.when((j > 0) & (j < n_tiles))
    def _():
        activate()
        raw[...] = dot32(n_s[...], w1_ref[...])
        acc[...] += dot32(hid[...], w2_ref[...])

    @pl.when(j == n_tiles)
    def _():
        activate()
        acc[...] += dot32(hid[...], w2_ref[...])
        finish()


def layers_kernel(n_tiles, own_ref, got_ref, w1_ref, w2_ref, o_ref, x_s, n_s, raw, hid, acc):
    layer, j = pl.program_id(0), pl.program_id(1)
    stage = lax.axis_index("pp")

    @pl.when((layer == 0) & (j == 0) & (stage == 0))
    def _():
        x_s[...] = own_ref[...]

    @pl.when((layer == 0) & (j == 0) & (stage != 0))
    def _():
        x_s[...] = got_ref[...]

    @pl.when(j == 0)
    def _():
        norm_rows(n_s, x_s)
        acc[...] = jnp.zeros_like(acc)

    def finish():
        for r in range(0, x_s.shape[0], GROUP):
            rs = slice(r, r + GROUP)
            out = (x_s[rs, :].astype(F32) + acc[rs, :]).astype(BF16)
            x_s[rs, :] = out
            o_ref[rs, :] = out

    ffn_steps(j, n_tiles, n_s, w1_ref, w2_ref, raw, hid, acc, finish)


def run_layers(own, own_block, got, rows, w_one, w_two):
    width = own.shape[1]
    _, n_layers, _, ffn = w_one.shape
    n_tiles = ffn // FFN_TILE
    whole = pl.BlockSpec((rows, width), lambda l, j: (0, 0))
    return pl.pallas_call(
        functools.partial(layers_kernel, n_tiles),
        out_shape=jax.ShapeDtypeStruct((rows, width), BF16),
        grid=(n_layers, n_tiles + 1),
        in_specs=[
            pl.BlockSpec((rows, width), lambda l, j: (own_block, 0)),
            whole,
            pl.BlockSpec((None, None, width, FFN_TILE), lambda l, j: (0, l, 0, jnp.minimum(j, n_tiles - 1))),
            pl.BlockSpec((None, None, FFN_TILE, width), lambda l, j: (0, l, jnp.maximum(j - 1, 0), 0)),
        ],
        out_specs=whole,
        scratch_shapes=[
            pltpu.VMEM((rows, width), BF16),
            pltpu.VMEM((rows, width), BF16),
            pltpu.VMEM((rows, FFN_TILE), F32),
            pltpu.VMEM((rows, FFN_TILE), BF16),
            pltpu.VMEM((rows, width), F32),
        ],
        compiler_params=pltpu.CompilerParams(dimension_semantics=("arbitrary", "arbitrary"), vmem_limit_bytes=VMEM_BYTES),
        cost_estimate=pl.CostEstimate(
            flops=4 * rows * width * ffn * n_layers, bytes_accessed=4 * width * ffn * n_layers, transcendentals=0
        ),
        name="layers",
    )(own, got, w_one, w_two)


def mtp_kernel(
    n_proj, n_tiles, h_ref, e_ref, gf_ref, gh_ref, ge_ref, gm_ref, wp_ref, w1_ref, w2_ref, o_ref,
    cat_s, z_s, n_s, raw, hid, acc,
):
    step = pl.program_id(0)
    rows, width = h_ref.shape
    proj_tile = wp_ref.shape[0]

    @pl.when(step == 0)
    def _():
        norm_rows(cat_s.at[:, pl.ds(0, width)], h_ref, gh_ref)
        norm_rows(cat_s.at[:, pl.ds(width, width)], e_ref, ge_ref)
        norm_rows(o_ref, h_ref, gf_ref)
        acc[...] = jnp.zeros_like(acc)

    @pl.when(step < n_proj)
    def _():
        at = pl.multiple_of(step * proj_tile, proj_tile)
        acc[...] += dot32(cat_s[:, pl.ds(at, proj_tile)], wp_ref[...])

    @pl.when(step == n_proj - 1)
    def _():
        for r in range(0, rows, GROUP):
            z_s[r:r + GROUP, :] = acc[r:r + GROUP, :].astype(BF16)
        norm_rows(n_s, z_s, gm_ref)
        acc[...] = jnp.zeros_like(acc)

    def finish():
        for r in range(0, rows, GROUP):
            rs = slice(r, r + GROUP)
            z_s[rs, :] = (z_s[rs, :].astype(F32) + acc[rs, :]).astype(BF16)
        norm_rows(o_ref, z_s, gf_ref, rows)

    ffn_steps(step - n_proj, n_tiles, n_s, w1_ref, w2_ref, raw, hid, acc, finish)


def run_mtp(h_last, e_rows, rows, gain_f, gain_h, gain_e, gain_m, w_proj, u_one, u_two):
    width = h_last.shape[1]
    ffn = u_one.shape[1]
    n_tiles = ffn // FFN_TILE
    n_proj = w_proj.shape[0] // FFN_TILE
    whole = pl.BlockSpec((rows, width), lambda s: (0, 0))
    gain = pl.BlockSpec((1, width), lambda s: (0, 0))
    return pl.pallas_call(
        functools.partial(mtp_kernel, n_proj, n_tiles),
        out_shape=jax.ShapeDtypeStruct((2 * rows, width), BF16),
        grid=(n_proj + n_tiles + 1,),
        in_specs=[
            whole, whole, gain, gain, gain, gain,
            pl.BlockSpec((FFN_TILE, width), lambda s: (jnp.minimum(s, n_proj - 1), 0)),
            pl.BlockSpec((width, FFN_TILE), lambda s: (0, jnp.clip(s - n_proj, 0, n_tiles - 1))),
            pl.BlockSpec((FFN_TILE, width), lambda s: (jnp.clip(s - n_proj - 1, 0, n_tiles - 1), 0)),
        ],
        out_specs=pl.BlockSpec((2 * rows, width), lambda s: (0, 0)),
        scratch_shapes=[
            pltpu.VMEM((rows, 2 * width), BF16),
            pltpu.VMEM((rows, width), BF16),
            pltpu.VMEM((rows, width), BF16),
            pltpu.VMEM((rows, FFN_TILE), F32),
            pltpu.VMEM((rows, FFN_TILE), BF16),
            pltpu.VMEM((rows, width), F32),
        ],
        compiler_params=pltpu.CompilerParams(dimension_semantics=("arbitrary",), vmem_limit_bytes=VMEM_BYTES),
        cost_estimate=pl.CostEstimate(
            flops=4 * rows * width * (ffn + width), bytes_accessed=4 * width * (ffn + width), transcendentals=0
        ),
        name="mtp",
    )(h_last, e_rows, gain_f[None], gain_h[None], gain_e[None], gain_m[None], w_proj, u_one, u_two)


def head_stats(buf, n_cols, base, tgt_ref, m_ref, s_ref, p_ref):
    rows = buf.shape[0]
    lane = lax.broadcasted_iota(jnp.int32, (GROUP, LANES), 1)
    for r in range(0, rows, GROUP):
        rs = slice(r, r + GROUP)
        parts = [buf[rs, c:c + LANES] for c in range(0, n_cols, LANES)]
        top = parts[0]
        for part in parts[1:]:
            top = jnp.maximum(top, part)
        m_old = m_ref[rs, :]
        m_new = jnp.maximum(m_old, top)
        total = s_ref[rs, :] * jnp.exp(m_old - m_new)
        rel = tgt_ref[rs, :] - lane - base
        pick = p_ref[rs, :]
        for k, part in enumerate(parts):
            total = total + jnp.exp(part - m_new)
            pick = jnp.where(rel == k * LANES, part, pick)
        m_ref[rs, :] = m_new
        s_ref[rs, :] = total
        p_ref[rs, :] = pick


def head_kernel(n_steps, tail, first, x_ref, tgt_ref, w_ref, o_ref, buf_a, buf_b, t_ref, m_ref, s_ref, p_ref):
    i = pl.program_id(0)
    half = buf_a.shape[1]
    rows = x_ref.shape[0] // 2
    n_seq = tgt_ref.shape[0] // 2
    state = (t_ref, m_ref, s_ref, p_ref)
    row = lax.broadcasted_iota(I32, (GROUP, LANES), 0)
    lane = lax.broadcasted_iota(I32, (GROUP, LANES), 1)

    @pl.when(i == 0)
    def _():
        buf_b[...] = jnp.full_like(buf_b, -3e38)
        m_ref[...] = jnp.full_like(m_ref, -3e38)
        s_ref[...] = jnp.zeros_like(s_ref)
        p_ref[...] = jnp.zeros_like(p_ref)
        for part in range(2):
            for r in range(0, rows, GROUP):
                want = jnp.zeros((GROUP, LANES), F32)
                for q in range(n_seq):
                    line = tgt_ref[part * n_seq + q:part * n_seq + q + 1, :].astype(F32)
                    want = want + jnp.where(q * LANES + lane == first + r + row, jnp.broadcast_to(line, want.shape), 0.0)
                want = jnp.sum(want, axis=1, keepdims=True)
                at = part * rows + r
                t_ref[at:at + GROUP, :] = jnp.broadcast_to(want, (GROUP, LANES)).astype(I32)

    @pl.when(i < n_steps - 1)
    def _():
        buf_a[...] = dot32(x_ref[...], w_ref[:, :half])
        head_stats(buf_b, half, (2 * i - 1) * half, *state)
        buf_b[...] = dot32(x_ref[...], w_ref[:, half:])
        head_stats(buf_a, half, 2 * i * half, *state)

    @pl.when(i == n_steps - 1)
    def _():
        head_stats(buf_b, half, (2 * i - 1) * half, *state)
        done = 0
        while done < tail:
            cols = min(half, tail - done)
            buf_a[:, :cols] = dot32(x_ref[...], w_ref[:, done:done + cols])
            head_stats(buf_a, cols, 2 * i * half + done, *state)
            done += cols
        for part in range(2):
            lines = [jnp.zeros((1, LANES), F32) for _ in range(n_seq)]
            for r in range(0, rows, GROUP):
                rs = slice(part * rows + r, part * rows + r + GROUP)
                top = jnp.max(m_ref[rs, :], axis=1, keepdims=True)
                total = jnp.sum(s_ref[rs, :] * jnp.exp(m_ref[rs, :] - top), axis=1, keepdims=True)
                picked = jnp.sum(p_ref[rs, :], axis=1, keepdims=True)
                nll = jnp.broadcast_to(top + jnp.log(total) - picked, (GROUP, LANES))
                for q in range(n_seq):
                    if q * LANES < first + r + GROUP and first + r < (q + 1) * LANES:
                        here = jnp.where(q * LANES + lane == first + r + row, nll, 0.0)
                        lines[q] = lines[q] + jnp.sum(here, axis=0, keepdims=True)
            o_ref[part * n_seq:(part + 1) * n_seq, :] = jnp.concatenate(lines, axis=0)


def run_head(x_val, tgt_tile, first, w_out):
    rows, width = x_val.shape
    vocab = w_out.shape[1]
    tile = 2 * HEAD_HALF
    n_steps = pl.cdiv(vocab, tile)
    tail = vocab - (n_steps - 1) * tile
    small = pl.BlockSpec(tgt_tile.shape, lambda i: (0, 0))
    return pl.pallas_call(
        functools.partial(head_kernel, n_steps, tail, first),
        out_shape=jax.ShapeDtypeStruct(tgt_tile.shape, F32),
        grid=(n_steps,),
        in_specs=[
            pl.BlockSpec((rows, width), lambda i: (0, 0)),
            small,
            pl.BlockSpec((width, tile), lambda i: (0, i)),
        ],
        out_specs=small,
        scratch_shapes=[pltpu.VMEM((rows, HEAD_HALF), F32)] * 2
        + [pltpu.VMEM((rows, LANES), I32)]
        + [pltpu.VMEM((rows, LANES), F32)] * 3,
        compiler_params=pltpu.CompilerParams(dimension_semantics=("arbitrary",), vmem_limit_bytes=VMEM_BYTES),
        cost_estimate=pl.CostEstimate(flops=2 * rows * width * vocab, bytes_accessed=2 * width * vocab, transcendentals=0),
        name="head",
    )(x_val, tgt_tile, w_out)


def solution(mesh):
    n_data = mesh.shape["dp"]
    n_stages = mesh.shape["pp"]

    def extra_rows(table, want, j):
        me = lax.axis_index("dp")
        n_local = table.shape[0]
        ids_all = lax.all_gather(want, "dp")
        held = ids_all // n_local == me
        rank = jnp.cumsum(held.astype(I32), axis=1) - 1
        slot = j * CAP + jnp.arange(CAP)
        hit = held[:, None, :] & (rank[:, None, :] == slot[None, :, None])
        idx = jnp.sum(jnp.where(hit, (ids_all - me * n_local)[:, None, :], 0), axis=2)
        packed = table[idx]
        got = lax.all_to_all(packed, "dp", 0, 0)
        owner = want // n_local
        mine = owner[:, None] == jnp.arange(n_data)[None, :]
        ranks = jnp.sum(jnp.where(mine, jnp.cumsum(mine.astype(I32), axis=0) - 1, 0), axis=1) - j * CAP
        place = jnp.where((ranks >= 0) & (ranks < CAP), owner * CAP + ranks, -1)
        pick = (place[:, None] == jnp.arange(n_data * CAP)[None, :]).astype(BF16)
        return dot32(pick, got.reshape(n_data * CAP, -1)).astype(BF16)

    def body(tok_ids, emb_s, w_one, w_two, gain_f, gain_h, gain_e, gain_m, w_proj, u_one, u_two, w_out):
        stage = lax.axis_index("pp")
        n_micro, batch_dev, seq_plus = tok_ids.shape
        seq_len = seq_plus - 2
        n_seq = n_micro * batch_dev
        n_tok = n_seq * seq_len
        assert seq_len == LANES and 2 * n_seq == BLOCK
        rows_a = ROWS_A
        rows_b = n_tok - rows_a
        table = emb_s[0]
        n_local = table.shape[0]
        ids = tok_ids.reshape(n_seq, seq_plus)
        spare = jnp.full((n_seq, seq_len - 1), -1, I32)
        ids_tile = jnp.concatenate([ids[:, :seq_len + 1], spare], axis=1).reshape(2 * n_seq, seq_len)
        tgt_tile = jnp.concatenate([ids[:, 1:seq_len + 1], ids[:, 2:]], axis=0)

        idx, most = run_slots(ids_tile, n_data, n_local)
        packed = run_pack(idx, table)
        x_all, e_all = run_trade(ids_tile, packed, n_local, n_seq, 2 * rows_a)

        def more(carry):
            j, x_val, e_val = carry
            rows = extra_rows(table, ids[:, :seq_len + 1].reshape(-1), j).reshape(n_seq, seq_len + 1, -1)
            x_more = rows[:, :seq_len].reshape(n_tok, -1)
            e_more = rows[:, 1:].reshape(n_tok, -1)
            return j + 1, x_val + jnp.pad(x_more, ((0, 2 * rows_a - n_tok), (0, 0))), e_val + e_more

        most = most[0, 0]
        _, x_all, e_all = lax.while_loop(lambda c: c[0] * CAP < most, more, (jnp.int32(1), x_all, e_all))

        x_mid = run_layers(x_all, 0, x_all, rows_a, w_one, w_two)
        moved, e_last = run_hand_on(x_mid, e_all)
        swapped = run_swap(run_layers(x_all, 1, moved, rows_a, w_one, w_two))

        def tail(h_last, e_rows, first, rows):
            normed = run_mtp(h_last, e_rows, rows, gain_f, gain_h, gain_e, gain_m, w_proj, u_one, u_two)
            return run_head(normed, tgt_tile, first, w_out)

        def tail_first():
            return tail(swapped, e_all, 0, rows_a)

        def tail_last():
            return tail(run_layers(swapped, 0, swapped, rows_b, w_one, w_two), e_last, rows_a, rows_b)

        tile = lax.cond(stage == 0, tail_first, tail_last)
        nll, total = run_finish(tile, n_data, n_stages, 1.0 / (n_tok * n_data))
        shape = (n_micro, batch_dev, seq_len)
        return total[0, 0], nll[:n_seq].reshape(shape), nll[n_seq:].reshape(shape)

    rep = P()
    in_specs = (P(None, "dp", None), P("pp", "dp", None), P("pp"), P("pp")) + (rep,) * 8
    out_specs = (rep, P(None, "dp", None), P(None, "dp", None))
    return jax.shard_map(body, mesh=mesh, in_specs=in_specs, out_specs=out_specs, check_vma=False)
```

```python
import functools

import jax
import jax.numpy as jnp
from jax import lax
from jax.experimental import pallas as pl
from jax.experimental.pallas import tpu as pltpu
from jax.sharding import PartitionSpec as P

NORM_EPS = 1e-6
MTP_WEIGHT = 0.3
F32 = jnp.float32
BF16 = jnp.bfloat16
I32 = jnp.int32
MESH = pl.DeviceIdType.MESH
VMEM_BYTES = 60 * 1024 * 1024
LANES = 128
GROUP = 16

ROWS_A = 288
FFN_TILE = 1024
HEAD_HALF = 1024
HEAD_PARTS = 4
CAP = 160
SLOTS = 3
BLOCK = 8


def rms(x_f):
    return x_f * lax.rsqrt(jnp.mean(x_f * x_f, axis=-1, keepdims=True) + NORM_EPS)


def rms_gain(x_val, gain_ref):
    return (rms(x_val.astype(F32)) * gain_ref[...].astype(F32)).astype(BF16)


def dot32(a, b):
    return jnp.dot(a, b, preferred_element_type=F32)


def norm_rows(dst, src, gain_ref=None, base=0):
    for r in range(0, src.shape[0], GROUP):
        val = rms(src[r:r + GROUP, :].astype(F32))
        if gain_ref is not None:
            val = val * gain_ref[...].astype(F32)
        dst[base + r:base + r + GROUP, :] = val.astype(BF16)


def collective(idx):
    return pltpu.CompilerParams(collective_id=idx, has_side_effects=True, vmem_limit_bytes=VMEM_BYTES)


def enter(peers):
    barrier = pltpu.get_barrier_semaphore()
    for peer in peers:
        pl.semaphore_signal(barrier, inc=1, device_id=peer, device_id_type=MESH)
    pl.semaphore_wait(barrier, len(peers))


def push(src, dst, send_sem, recv_sem, peer):
    return pltpu.make_async_remote_copy(
        src_ref=src, dst_ref=dst, send_sem=send_sem, recv_sem=recv_sem, device_id=peer, device_id_type=MESH
    )


def slot_ranks(held):
    row = lax.broadcasted_iota(I32, (LANES, LANES), 0)
    col = lax.broadcasted_iota(I32, (LANES, LANES), 1)
    ahead = dot32(held.astype(BF16), (row < col).astype(BF16))
    total = dot32(held.astype(BF16), jnp.ones((LANES, LANES), BF16))
    out, base = [], jnp.zeros((1, LANES), F32)
    for r in range(held.shape[0]):
        out.append(ahead[r:r + 1, :] + base)
        base = base + total[r:r + 1, :]
    return jnp.concatenate(out, axis=0)


def slots_kernel(n_data, n_local, ids_ref, idx_ref, most_ref, all_ref, got, send_sem, recv_sem):
    me, stage = lax.axis_index("dp"), lax.axis_index("pp")
    peers = [(jnp.bitwise_xor(me, k), stage) for k in range(1, n_data)]
    enter(peers)
    copies = [push(ids_ref, got.at[k], send_sem.at[k], recv_sem.at[k], peer) for k, peer in enumerate(peers)]
    for copy in copies:
        copy.start()
    for copy in copies:
        copy.wait()
    most = jnp.zeros((1, 1), F32)
    slot = lax.broadcasted_iota(I32, (CAP, LANES), 0).astype(F32)
    for k in range(n_data):
        ids = ids_ref[...] if k == 0 else got[k - 1]
        all_ref[k] = ids
        for s in range(n_data):
            inside = ((ids >= s * n_local) & (ids < (s + 1) * n_local)).astype(F32)
            most = jnp.maximum(most, jnp.sum(jnp.sum(inside, axis=1, keepdims=True), axis=0, keepdims=True))
        local = ids - me * n_local
        held = ((local >= 0) & (local < n_local)).astype(F32)
        rank = jnp.where(held > 0, slot_ranks(held), -1.0)
        high = lax.shift_right_arithmetic(local, 8)
        low = (local - high * 256).astype(F32)
        high = high.astype(F32)
        acc = jnp.zeros((BLOCK, CAP), F32)
        for r in range(ids.shape[0]):
            hit = (jnp.broadcast_to(rank[r:r + 1, :], (CAP, LANES)) == slot).astype(BF16)
            keep = held[r:r + 1, :]
            pair = jnp.concatenate(
                [high[r:r + 1, :] * keep, low[r:r + 1, :] * keep, jnp.zeros((BLOCK - 2, LANES), F32)], axis=0
            ).astype(BF16)
            acc = acc + lax.dot_general(pair, hit, (((1,), (1,)), ((), ())), preferred_element_type=F32)
        idx_ref[k:k + 1, :CAP] = (acc[0:1, :] * 256.0 + acc[1:2, :]).astype(I32)
    most_ref[...] = jnp.broadcast_to(most, most_ref.shape).astype(I32)


def run_slots(ids_tile, n_data, n_local):
    vmem = pl.BlockSpec(memory_space=pltpu.VMEM)
    return pl.pallas_call(
        functools.partial(slots_kernel, n_data, n_local),
        out_shape=[jax.ShapeDtypeStruct((n_data, 2 * LANES), I32), jax.ShapeDtypeStruct((BLOCK, LANES), I32),
                   jax.ShapeDtypeStruct((n_data, BLOCK, LANES), I32)],
        in_specs=[vmem],
        out_specs=[vmem, vmem, vmem],
        scratch_shapes=[
            pltpu.VMEM((n_data - 1, BLOCK, LANES), I32),
            pltpu.SemaphoreType.DMA((n_data - 1,)),
            pltpu.SemaphoreType.DMA((n_data - 1,)),
        ],
        compiler_params=collective(0),
        name="slots",
    )(ids_tile)


def pack_kernel(n_data, idx_ref, lane_ref, table_ref, o_ref, held, sems):
    parts = [(0, LANES), (LANES, CAP - LANES)]

    @pl.when(lax.axis_index("pp") == 0)
    def _():
        for k in range(n_data):
            for p, (first, count) in enumerate(parts):
                def fetch(c, carry):
                    start = pl.multiple_of(lax.shift_right_logical(idx_ref[k, first + c], 3) * BLOCK, BLOCK)
                    to = pl.multiple_of((k * CAP + first + c) * BLOCK, BLOCK)
                    pltpu.make_async_copy(
                        table_ref.at[pl.ds(start, BLOCK), :], held.at[pl.ds(to, BLOCK), :], sems.at[k * 2 + p]
                    ).start()
                    return carry

                lax.fori_loop(0, count, fetch, 0, unroll=8)
        for k in range(n_data):
            for p, (first, count) in enumerate(parts):
                at = (k * CAP + first) * BLOCK
                span = count * BLOCK
                pltpu.make_async_copy(table_ref.at[pl.ds(0, span), :], held.at[pl.ds(at, span), :], sems.at[k * 2 + p]).wait()
                idx = jnp.broadcast_to(lane_ref[k:k + 1, p * LANES:(p + 1) * LANES].astype(F32), (LANES, LANES))
                idx = jnp.transpose(idx)[:count, :].astype(I32)
                low = jnp.bitwise_and(idx, BLOCK - 1)
                row = lax.broadcasted_iota(I32, (count, LANES), 0)
                lane = lax.broadcasted_iota(I32, (count, LANES), 1)
                picks = []
                for c in range(0, span, LANES):
                    at_row = c // BLOCK + lax.shift_right_logical(lane, 3)
                    picks.append(((row == at_row) & (low == jnp.bitwise_and(lane, BLOCK - 1))).astype(F32).astype(BF16))
                pick = jnp.concatenate(picks, axis=1)
                o_ref[k, first:first + count, :] = dot32(pick, held[at:at + span, :]).astype(BF16)


def run_pack(idx, table):
    n_data = idx.shape[0]
    width = table.shape[1]
    return pl.pallas_call(
        functools.partial(pack_kernel, n_data),
        out_shape=jax.ShapeDtypeStruct((n_data, CAP, width), BF16),
        in_specs=[
            pl.BlockSpec(memory_space=pltpu.SMEM),
            pl.BlockSpec(memory_space=pltpu.VMEM),
            pl.BlockSpec(memory_space=pl.ANY),
        ],
        out_specs=pl.BlockSpec(memory_space=pltpu.VMEM),
        scratch_shapes=[pltpu.VMEM((n_data * CAP * BLOCK, width), BF16), pltpu.SemaphoreType.DMA((2 * n_data,))],
        compiler_params=pltpu.CompilerParams(vmem_limit_bytes=VMEM_BYTES),
        name="pack",
    )(idx, idx, table)


def trade_kernel(n_data, n_local, n_seq, ids_ref, packed_ref, x_ref, e_ref, got, pick_s, send_sem, recv_sem):
    me, stage = lax.axis_index("dp"), lax.axis_index("pp")
    n_tok = n_seq * LANES
    if x_ref.shape[0] > n_tok:
        x_ref[n_tok:, :] = jnp.zeros((x_ref.shape[0] - n_tok, x_ref.shape[1]), BF16)

    @pl.when(stage == 0)
    def _():
        peers = [(jnp.bitwise_xor(me, k), stage) for k in range(1, n_data)]
        enter(peers)
        copies = [
            push(packed_ref.at[k + 1], got.at[k], send_sem.at[k], recv_sem.at[k], peer) for k, peer in enumerate(peers)
        ]
        for k in (2, 0, 1):
            copies[k].start()
        ids = ids_ref[...]
        slot = lax.broadcasted_iota(I32, (CAP, LANES), 0).astype(F32)
        lane = lax.broadcasted_iota(I32, (1, LANES), 1)
        for k in range(n_data):
            src = jnp.bitwise_xor(me, k)
            held = ((ids >= src * n_local) & (ids < (src + 1) * n_local)).astype(F32)
            rank = jnp.where(held > 0, slot_ranks(held), -1.0)
            ahead = pltpu.roll(rank, LANES - 1, 1)
            for s in range(n_seq):
                now = rank[2 * s:2 * s + 1, :]
                later = jnp.where(lane == LANES - 1, ahead[2 * s + 1:2 * s + 2, :], ahead[2 * s:2 * s + 1, :])
                for q, want in ((s, now), (n_seq + s, later)):
                    hit = (jnp.broadcast_to(want, (CAP, LANES)) == slot).astype(F32).astype(BF16)
                    pick_s[k * CAP:(k + 1) * CAP, q * LANES:(q + 1) * LANES] = hit

        def placed(k, block):
            return lax.dot_general(
                pick_s[k * CAP:(k + 1) * CAP, :], block, (((0,), (0,)), ((), ())), preferred_element_type=F32
            ).astype(BF16)

        def add(val):
            x_ref[:n_tok, :] += val[:n_tok]
            e_ref[:n_tok, :] += val[n_tok:]

        first = placed(0, packed_ref[0])
        x_ref[:n_tok, :] = first[:n_tok]
        e_ref[:n_tok, :] = first[n_tok:]
        for k in (2, 0, 1):
            copies[k].wait()
            add(placed(k + 1, got[k]))

    @pl.when(stage != 0)
    def _():
        x_ref[:n_tok, :] = jnp.zeros((n_tok, x_ref.shape[1]), BF16)
        e_ref[:n_tok, :] = jnp.zeros((n_tok, x_ref.shape[1]), BF16)


def run_trade(ids_tile, packed, n_local, n_seq, pad_rows):
    n_data, _, width = packed.shape
    n_tok = n_seq * LANES
    vmem = pl.BlockSpec(memory_space=pltpu.VMEM)
    return pl.pallas_call(
        functools.partial(trade_kernel, n_data, n_local, n_seq),
        out_shape=[jax.ShapeDtypeStruct((pad_rows, width), BF16), jax.ShapeDtypeStruct((n_tok, width), BF16)],
        in_specs=[vmem, vmem],
        out_specs=[vmem, vmem],
        scratch_shapes=[
            pltpu.VMEM((n_data - 1, CAP, width), BF16),
            pltpu.VMEM((n_data * CAP, 2 * n_tok), BF16),
            pltpu.SemaphoreType.DMA((n_data - 1,)),
            pltpu.SemaphoreType.DMA((n_data - 1,)),
        ],
        compiler_params=collective(1),
        name="trade",
    )(ids_tile, packed)


def hand_on_kernel(rows_a, x_ref, e_ref, x_out, e_out, send_sem, recv_sem):
    me, stage = lax.axis_index("dp"), lax.axis_index("pp")
    peer = (me, 1 - stage)
    enter([peer])
    copies = [
        push(x_ref, x_out, send_sem.at[0], recv_sem.at[0], peer),
        push(e_ref.at[pl.ds(rows_a, e_out.shape[0]), :], e_out, send_sem.at[1], recv_sem.at[1], peer),
    ]

    @pl.when(stage == 0)
    def _():
        for copy in copies:
            copy.start()
        for copy in copies:
            copy.wait_send()

    @pl.when(stage != 0)
    def _():
        for copy in copies:
            copy.wait_recv()


def run_hand_on(x_val, e_val):
    rows_a, width = x_val.shape
    rows_b = e_val.shape[0] - rows_a
    hbm = pl.BlockSpec(memory_space=pl.ANY)
    return pl.pallas_call(
        functools.partial(hand_on_kernel, rows_a),
        out_shape=[jax.ShapeDtypeStruct((rows_a, width), BF16), jax.ShapeDtypeStruct((rows_b, width), BF16)],
        in_specs=[hbm, hbm],
        out_specs=[hbm, hbm],
        scratch_shapes=[pltpu.SemaphoreType.DMA((2,)), pltpu.SemaphoreType.DMA((2,))],
        compiler_params=collective(2),
        name="hand_on",
    )(x_val, e_val)


def swap_kernel(x_ref, o_ref, send_sem, recv_sem):
    peer = (lax.axis_index("dp"), 1 - lax.axis_index("pp"))
    enter([peer])
    copy = push(x_ref, o_ref, send_sem, recv_sem, peer)
    copy.start()
    copy.wait()


def run_swap(x_val):
    hbm = pl.BlockSpec(memory_space=pl.ANY)
    return pl.pallas_call(
        swap_kernel,
        out_shape=jax.ShapeDtypeStruct(x_val.shape, BF16),
        in_specs=[hbm],
        out_specs=hbm,
        scratch_shapes=[pltpu.SemaphoreType.DMA, pltpu.SemaphoreType.DMA],
        compiler_params=collective(3),
        name="swap",
    )(x_val)


def finish_kernel(n_data, n_stages, scale, x_ref, nll_ref, total_ref, got, send_sem, recv_sem):
    me, stage = lax.axis_index("dp"), lax.axis_index("pp")
    mine = me * n_stages + stage
    steps = [(k, c) for k in range(n_data) for c in range(n_stages) if (k, c) != (0, 0)]
    peers = [(jnp.bitwise_xor(me, k), jnp.bitwise_xor(stage, c)) for k, c in steps]
    enter(peers)
    copies = [push(x_ref, got.at[mine], send_sem.at[i], recv_sem.at[i], peer) for i, peer in enumerate(peers)]
    for copy in copies:
        copy.start()
    for copy in copies:
        copy.wait()
    got[mine] = x_ref[...]
    half = x_ref.shape[0] // 2
    total = jnp.zeros(x_ref.shape, F32)
    for i in range(n_data * n_stages):
        total = total + got[i]
    main = jnp.sum(jnp.sum(total[:half], axis=1, keepdims=True), axis=0, keepdims=True)
    mtp = jnp.sum(jnp.sum(total[half:], axis=1, keepdims=True), axis=0, keepdims=True)
    total_ref[...] = jnp.broadcast_to((main + MTP_WEIGHT * mtp) * scale, total_ref.shape)
    nll = x_ref[...]
    for c in range(1, n_stages):
        nll = nll + got[me * n_stages + jnp.bitwise_xor(stage, c)]
    nll_ref[...] = nll


def run_finish(tile, n_data, n_stages, scale):
    vmem = pl.BlockSpec(memory_space=pltpu.VMEM)
    n_peers = n_data * n_stages - 1
    return pl.pallas_call(
        functools.partial(finish_kernel, n_data, n_stages, scale),
        out_shape=[jax.ShapeDtypeStruct(tile.shape, F32), jax.ShapeDtypeStruct(tile.shape, F32)],
        in_specs=[vmem],
        out_specs=[vmem, vmem],
        scratch_shapes=[
            pltpu.VMEM((n_data * n_stages,) + tile.shape, F32),
            pltpu.SemaphoreType.DMA((n_peers,)),
            pltpu.SemaphoreType.DMA((n_peers,)),
        ],
        compiler_params=collective(4),
        name="finish",
    )(tile)


def ring_copy(src, ring, sems, i):
    slot = lax.rem(i, SLOTS)
    return pltpu.make_async_copy(src, ring.at[slot], sems.at[slot])


def ffn_steps(j, n_tiles, n_s, w1_slot, w2_slot, ring1, ring2, raw, hid, acc, finish):
    def activate():
        for r in range(0, raw.shape[0], GROUP):
            for c in range(0, raw.shape[1], 2 * LANES):
                spot = (slice(r, r + GROUP), slice(c, c + 2 * LANES))
                hid[spot] = jax.nn.gelu(raw[spot]).astype(BF16)

    @pl.when(j == 0)
    def _():
        raw[...] = dot32(n_s[...], ring1[w1_slot])

    @pl.when((j > 0) & (j < n_tiles))
    def _():
        activate()
        raw[...] = dot32(n_s[...], ring1[w1_slot])
        acc[...] += dot32(hid[...], ring2[w2_slot])

    @pl.when(j == n_tiles)
    def _():
        activate()
        acc[...] += dot32(hid[...], ring2[w2_slot])
        finish()


def layers_kernel(n_tiles, n_layers, own_ref, got_ref, w1_hbm, w2_hbm, o_ref, x_s, n_s, raw, hid, acc, ring1, ring2, sem1, sem2):
    layer, j = pl.program_id(0), pl.program_id(1)
    stage = lax.axis_index("pp")
    total = n_layers * n_tiles
    up, down = layer * n_tiles + j, layer * n_tiles + j - 1

    def copy1(i):
        col = pl.multiple_of(lax.rem(i, n_tiles) * FFN_TILE, FFN_TILE)
        return ring_copy(w1_hbm.at[0, lax.div(i, n_tiles), :, pl.ds(col, FFN_TILE)], ring1, sem1, i)

    def copy2(i):
        row = pl.multiple_of(lax.rem(i, n_tiles) * FFN_TILE, FFN_TILE)
        return ring_copy(w2_hbm.at[0, lax.div(i, n_tiles), pl.ds(row, FFN_TILE), :], ring2, sem2, i)

    start = (layer == 0) & (j == 0)

    @pl.when(start)
    def _():
        copy1(0).start()

    @pl.when(start & (stage == 0))
    def _():
        x_s[...] = own_ref[...]

    @pl.when(start & (stage != 0))
    def _():
        x_s[...] = got_ref[...]

    @pl.when(j == 0)
    def _():
        norm_rows(n_s, x_s)
        acc[...] = jnp.zeros_like(acc)

    @pl.when(start)
    def _():
        copy1(1).start()
        copy2(0).start()
        copy2(1).start()

    @pl.when(j < n_tiles)
    def _():
        copy1(up).wait()

        @pl.when(up + SLOTS - 1 < total)
        def _():
            copy1(up + SLOTS - 1).start()

    @pl.when(j > 0)
    def _():
        copy2(down).wait()

        @pl.when(down + SLOTS - 1 < total)
        def _():
            copy2(down + SLOTS - 1).start()

    def finish():
        for r in range(0, x_s.shape[0], GROUP):
            rs = slice(r, r + GROUP)
            out = (x_s[rs, :].astype(F32) + acc[rs, :]).astype(BF16)
            x_s[rs, :] = out
            o_ref[rs, :] = out

    ffn_steps(
        j, n_tiles, n_s, lax.rem(up, SLOTS), lax.rem(jnp.maximum(down, 0), SLOTS), ring1, ring2, raw, hid, acc, finish
    )


def ring_scratch(width):
    return [
        pltpu.VMEM((SLOTS, width, FFN_TILE), BF16),
        pltpu.VMEM((SLOTS, FFN_TILE, width), BF16),
        pltpu.SemaphoreType.DMA((SLOTS,)),
        pltpu.SemaphoreType.DMA((SLOTS,)),
    ]


def run_layers(own, own_block, got, rows, w_one, w_two):
    width = own.shape[1]
    _, n_layers, _, ffn = w_one.shape
    n_tiles = ffn // FFN_TILE
    whole = pl.BlockSpec((rows, width), lambda l, j: (0, 0))
    hbm = pl.BlockSpec(memory_space=pl.ANY)
    return pl.pallas_call(
        functools.partial(layers_kernel, n_tiles, n_layers),
        out_shape=jax.ShapeDtypeStruct((rows, width), BF16),
        grid=(n_layers, n_tiles + 1),
        in_specs=[pl.BlockSpec((rows, width), lambda l, j: (own_block, 0)), whole, hbm, hbm],
        out_specs=whole,
        scratch_shapes=[
            pltpu.VMEM((rows, width), BF16),
            pltpu.VMEM((rows, width), BF16),
            pltpu.VMEM((rows, FFN_TILE), F32),
            pltpu.VMEM((rows, FFN_TILE), BF16),
            pltpu.VMEM((rows, width), F32),
        ] + ring_scratch(width),
        compiler_params=pltpu.CompilerParams(dimension_semantics=("arbitrary", "arbitrary"), vmem_limit_bytes=VMEM_BYTES),
        cost_estimate=pl.CostEstimate(
            flops=4 * rows * width * ffn * n_layers, bytes_accessed=4 * width * ffn * n_layers, transcendentals=0
        ),
        name="layers",
    )(own, got, w_one, w_two)


def mtp_kernel(
    n_proj, n_tiles, h_ref, e_ref, gf_ref, gh_ref, ge_ref, gm_ref, wp_hbm, w1_hbm, w2_hbm, o_ref,
    cat_s, z_s, n_s, raw, hid, acc, ring1, ring2, sem1, sem2,
):
    step = pl.program_id(0)
    rows, width = h_ref.shape
    j = step - n_proj
    total2 = n_proj + n_tiles
    second = jnp.where(step < n_proj, step, step - 1)

    def copy1(i):
        col = pl.multiple_of(i * FFN_TILE, FFN_TILE)
        return ring_copy(w1_hbm.at[:, pl.ds(col, FFN_TILE)], ring1, sem1, i)

    def copy2(src, i, tile):
        row = pl.multiple_of(tile * FFN_TILE, FFN_TILE)
        return ring_copy(src.at[pl.ds(row, FFN_TILE), :], ring2, sem2, i)

    def feed2(i):
        @pl.when(i < n_proj)
        def _():
            copy2(wp_hbm, i, i).start()

        @pl.when((i >= n_proj) & (i < total2))
        def _():
            copy2(w2_hbm, i, i - n_proj).start()

    @pl.when(step == 0)
    def _():
        copy2(wp_hbm, 0, 0).start()
        norm_rows(cat_s.at[:, pl.ds(0, width)], h_ref, gh_ref)
        norm_rows(cat_s.at[:, pl.ds(width, width)], e_ref, ge_ref)
        norm_rows(o_ref, h_ref, gf_ref)
        acc[...] = jnp.zeros_like(acc)
        copy2(wp_hbm, 1, 1).start()

    @pl.when(step == n_proj - 2)
    def _():
        copy1(0).start()
        copy1(1).start()

    @pl.when(j != 0)
    def _():
        copy2(wp_hbm, second, 0).wait()
        feed2(second + SLOTS - 1)

    @pl.when((j >= 0) & (j < n_tiles))
    def _():
        copy1(j).wait()

        @pl.when(j + SLOTS - 1 < n_tiles)
        def _():
            copy1(j + SLOTS - 1).start()

    @pl.when(step < n_proj)
    def _():
        at = pl.multiple_of(step * FFN_TILE, FFN_TILE)
        acc[...] += dot32(cat_s[:, pl.ds(at, FFN_TILE)], ring2[lax.rem(second, SLOTS)])

    @pl.when(step == n_proj - 1)
    def _():
        for r in range(0, rows, GROUP):
            z_s[r:r + GROUP, :] = acc[r:r + GROUP, :].astype(BF16)
        norm_rows(n_s, z_s, gm_ref)
        acc[...] = jnp.zeros_like(acc)

    def finish():
        for r in range(0, rows, GROUP):
            rs = slice(r, r + GROUP)
            z_s[rs, :] = (z_s[rs, :].astype(F32) + acc[rs, :]).astype(BF16)
        norm_rows(o_ref, z_s, gf_ref, rows)

    ffn_steps(
        j, n_tiles, n_s, lax.rem(jnp.maximum(j, 0), SLOTS), lax.rem(second, SLOTS), ring1, ring2, raw, hid, acc, finish
    )


def run_mtp(h_last, e_rows, rows, gain_f, gain_h, gain_e, gain_m, w_proj, u_one, u_two):
    width = h_last.shape[1]
    ffn = u_one.shape[1]
    n_tiles = ffn // FFN_TILE
    n_proj = w_proj.shape[0] // FFN_TILE
    whole = pl.BlockSpec((rows, width), lambda s: (0, 0))
    gain = pl.BlockSpec((1, width), lambda s: (0, 0))
    return pl.pallas_call(
        functools.partial(mtp_kernel, n_proj, n_tiles),
        out_shape=jax.ShapeDtypeStruct((2 * rows, width), BF16),
        grid=(n_proj + n_tiles + 1,),
        in_specs=[
            whole, whole, gain, gain, gain, gain,
            pl.BlockSpec(memory_space=pl.ANY), pl.BlockSpec(memory_space=pl.ANY), pl.BlockSpec(memory_space=pl.ANY),
        ],
        out_specs=pl.BlockSpec((2 * rows, width), lambda s: (0, 0)),
        scratch_shapes=[
            pltpu.VMEM((rows, 2 * width), BF16),
            pltpu.VMEM((rows, width), BF16),
            pltpu.VMEM((rows, width), BF16),
            pltpu.VMEM((rows, FFN_TILE), F32),
            pltpu.VMEM((rows, FFN_TILE), BF16),
            pltpu.VMEM((rows, width), F32),
        ] + ring_scratch(width),
        compiler_params=pltpu.CompilerParams(dimension_semantics=("arbitrary",), vmem_limit_bytes=VMEM_BYTES),
        cost_estimate=pl.CostEstimate(
            flops=4 * rows * width * (ffn + width), bytes_accessed=4 * width * (ffn + width), transcendentals=0
        ),
        name="mtp",
    )(h_last, e_rows, gain_f[None], gain_h[None], gain_e[None], gain_m[None], w_proj, u_one, u_two)


def head_stats(buf, n_cols, base, tgt_ref, m_ref, s_ref, p_ref):
    rows = buf.shape[0]
    lane = lax.broadcasted_iota(jnp.int32, (GROUP, LANES), 1)
    for r in range(0, rows, GROUP):
        rs = slice(r, r + GROUP)
        parts = [buf[rs, c:c + LANES] for c in range(0, n_cols, LANES)]
        top = parts[0]
        for part in parts[1:]:
            top = jnp.maximum(top, part)
        m_old = m_ref[rs, :]
        m_new = jnp.maximum(m_old, top)
        total = s_ref[rs, :] * jnp.exp(m_old - m_new)
        rel = tgt_ref[rs, :] - lane - base
        pick = p_ref[rs, :]
        for k, part in enumerate(parts):
            total = total + jnp.exp(part - m_new)
            pick = jnp.where(rel == k * LANES, part, pick)
        m_ref[rs, :] = m_new
        s_ref[rs, :] = total
        p_ref[rs, :] = pick


def head_kernel(n_steps, tail, first, x_ref, tgt_ref, w_ref, o_ref, buf_a, buf_b, t_ref, m_ref, s_ref, p_ref):
    i = pl.program_id(0)
    half = buf_a.shape[1]
    rows = x_ref.shape[0] // 2
    n_seq = tgt_ref.shape[0] // 2
    state = (t_ref, m_ref, s_ref, p_ref)
    row = lax.broadcasted_iota(I32, (GROUP, LANES), 0)
    lane = lax.broadcasted_iota(I32, (GROUP, LANES), 1)

    @pl.when(i == 0)
    def _():
        buf_b[...] = jnp.full_like(buf_b, -3e38)
        m_ref[...] = jnp.full_like(m_ref, -3e38)
        s_ref[...] = jnp.zeros_like(s_ref)
        p_ref[...] = jnp.zeros_like(p_ref)
        for part in range(2):
            for r in range(0, rows, GROUP):
                want = jnp.zeros((GROUP, LANES), F32)
                for q in range(n_seq):
                    line = tgt_ref[part * n_seq + q:part * n_seq + q + 1, :].astype(F32)
                    want = want + jnp.where(q * LANES + lane == first + r + row, jnp.broadcast_to(line, want.shape), 0.0)
                want = jnp.sum(want, axis=1, keepdims=True)
                at = part * rows + r
                t_ref[at:at + GROUP, :] = jnp.broadcast_to(want, (GROUP, LANES)).astype(I32)

    @pl.when(i < n_steps - 1)
    def _():
        bufs = (buf_a, buf_b)
        for q in range(HEAD_PARTS):
            bufs[q % 2][...] = dot32(x_ref[...], w_ref[:, q * half:(q + 1) * half])
            head_stats(bufs[(q + 1) % 2], half, (HEAD_PARTS * i + q - 1) * half, *state)

    @pl.when(i == n_steps - 1)
    def _():
        head_stats(buf_b, half, (HEAD_PARTS * i - 1) * half, *state)
        done = 0
        while done < tail:
            cols = min(half, tail - done)
            buf_a[:, :cols] = dot32(x_ref[...], w_ref[:, done:done + cols])
            head_stats(buf_a, cols, HEAD_PARTS * i * half + done, *state)
            done += cols
        for part in range(2):
            lines = [jnp.zeros((1, LANES), F32) for _ in range(n_seq)]
            for r in range(0, rows, GROUP):
                rs = slice(part * rows + r, part * rows + r + GROUP)
                top = jnp.max(m_ref[rs, :], axis=1, keepdims=True)
                total = jnp.sum(s_ref[rs, :] * jnp.exp(m_ref[rs, :] - top), axis=1, keepdims=True)
                picked = jnp.sum(p_ref[rs, :], axis=1, keepdims=True)
                nll = jnp.broadcast_to(top + jnp.log(total) - picked, (GROUP, LANES))
                for q in range(n_seq):
                    if q * LANES < first + r + GROUP and first + r < (q + 1) * LANES:
                        here = jnp.where(q * LANES + lane == first + r + row, nll, 0.0)
                        lines[q] = lines[q] + jnp.sum(here, axis=0, keepdims=True)
            o_ref[part * n_seq:(part + 1) * n_seq, :] = jnp.concatenate(lines, axis=0)


def run_head(x_val, tgt_tile, first, w_out):
    rows, width = x_val.shape
    vocab = w_out.shape[1]
    tile = HEAD_PARTS * HEAD_HALF
    n_steps = pl.cdiv(vocab, tile)
    tail = vocab - (n_steps - 1) * tile
    small = pl.BlockSpec(tgt_tile.shape, lambda i: (0, 0))
    return pl.pallas_call(
        functools.partial(head_kernel, n_steps, tail, first),
        out_shape=jax.ShapeDtypeStruct(tgt_tile.shape, F32),
        grid=(n_steps,),
        in_specs=[
            pl.BlockSpec((rows, width), lambda i: (0, 0)),
            small,
            pl.BlockSpec((width, tile), lambda i: (0, i)),
        ],
        out_specs=small,
        scratch_shapes=[pltpu.VMEM((rows, HEAD_HALF), F32)] * 2
        + [pltpu.VMEM((rows, LANES), I32)]
        + [pltpu.VMEM((rows, LANES), F32)] * 3,
        compiler_params=pltpu.CompilerParams(dimension_semantics=("arbitrary",), vmem_limit_bytes=VMEM_BYTES),
        cost_estimate=pl.CostEstimate(flops=2 * rows * width * vocab, bytes_accessed=2 * width * vocab, transcendentals=0),
        name="head",
    )(x_val, tgt_tile, w_out)


def solution(mesh):
    n_data = mesh.shape["dp"]
    n_stages = mesh.shape["pp"]

    def swap_perm(k):
        return [(d * n_stages, (d ^ k) * n_stages) for d in range(n_data)]

    def extra_rows(table, ids_all, j):
        me = lax.axis_index("dp")
        n_local = table.shape[0]
        ids_all = jnp.where(j > 0, ids_all, 0)
        n = ids_all.shape[1]
        before = (jnp.arange(n)[:, None] < jnp.arange(n)[None, :]).astype(BF16)
        owner = ids_all // n_local

        def ranks(held):
            return dot32(held.astype(BF16), before).astype(I32) - j * CAP

        held = owner == me
        hit = held[:, None, :] & (ranks(held)[:, None, :] == jnp.arange(CAP)[None, :, None])
        idx = jnp.sum(jnp.where(hit, (ids_all - me * n_local)[:, None, :], 0), axis=2)
        got = [table[idx[0]]] + [lax.ppermute(table[idx[k]], ("dp", "pp"), swap_perm(k)) for k in range(1, n_data)]
        src = jnp.bitwise_xor(owner[0], me)
        mine = src[None, :] == jnp.arange(n_data)[:, None]
        rank = jnp.sum(jnp.where(mine, ranks(mine), 0), axis=0)
        place = jnp.where((rank >= 0) & (rank < CAP), src * CAP + rank, -1)
        pick = (place[:, None] == jnp.arange(n_data * CAP)[None, :]).astype(BF16)
        return dot32(pick, jnp.concatenate(got, axis=0)).astype(BF16)

    def body(tok_ids, emb_s, w_one, w_two, gain_f, gain_h, gain_e, gain_m, w_proj, u_one, u_two, w_out):
        stage = lax.axis_index("pp")
        n_micro, batch_dev, seq_plus = tok_ids.shape
        seq_len = seq_plus - 2
        n_seq = n_micro * batch_dev
        n_tok = n_seq * seq_len
        assert seq_len == LANES and 2 * n_seq == BLOCK
        rows_a = ROWS_A
        rows_b = n_tok - rows_a
        table = emb_s[0]
        n_local = table.shape[0]
        ids = tok_ids.reshape(n_seq, seq_plus)
        spare = jnp.full((n_seq, seq_len - 1), -1, I32)
        ids_tile = jnp.concatenate([ids[:, :seq_len + 1], spare], axis=1).reshape(2 * n_seq, seq_len)
        tgt_tile = jnp.concatenate([ids[:, 1:seq_len + 1], ids[:, 2:]], axis=0)

        idx, most, ids_seen = run_slots(ids_tile, n_data, n_local)
        packed = run_pack(idx, table)
        x_all, e_all = run_trade(ids_tile, packed, n_local, n_seq, 2 * rows_a)

        def more(carry):
            j, x_val, e_val = carry
            wanted = ids_seen.reshape(n_data, n_seq, 2 * seq_len)[:, :, :seq_len + 1].reshape(n_data, -1)
            rows = extra_rows(table, wanted, j).reshape(n_seq, seq_len + 1, -1)
            x_more = rows[:, :seq_len].reshape(n_tok, -1)
            e_more = rows[:, 1:].reshape(n_tok, -1)
            return j + 1, x_val + jnp.pad(x_more, ((0, 2 * rows_a - n_tok), (0, 0))), e_val + e_more

        most = most[0, 0]
        _, x_all, e_all = lax.while_loop(lambda c: c[0] * CAP < most, more, (jnp.int32(1), x_all, e_all))

        x_mid = run_layers(x_all, 0, x_all, rows_a, w_one, w_two)
        moved, e_last = run_hand_on(x_mid, e_all)
        swapped = run_swap(run_layers(x_all, 1, moved, rows_a, w_one, w_two))

        def tail(h_last, e_rows, first, rows):
            normed = run_mtp(h_last, e_rows, rows, gain_f, gain_h, gain_e, gain_m, w_proj, u_one, u_two)
            return run_head(normed, tgt_tile, first, w_out)

        def tail_first():
            return tail(swapped, e_all, 0, rows_a)

        def tail_last():
            return tail(run_layers(swapped, 0, swapped, rows_b, w_one, w_two), e_last, rows_a, rows_b)

        tile = lax.cond(stage == 0, tail_first, tail_last)
        nll, total = run_finish(tile, n_data, n_stages, 1.0 / (n_tok * n_data))
        shape = (n_micro, batch_dev, seq_len)
        return total[0, 0], nll[:n_seq].reshape(shape), nll[n_seq:].reshape(shape)

    rep = P()
    in_specs = (P(None, "dp", None), P("pp", "dp", None), P("pp"), P("pp")) + (rep,) * 8
    out_specs = (rep, P(None, "dp", None), P(None, "dp", None))
    return jax.shard_map(body, mesh=mesh, in_specs=in_specs, out_specs=out_specs, check_vma=False)
```

```python
import functools

import jax
import jax.numpy as jnp
from jax import lax
from jax.experimental import pallas as pl
from jax.experimental.pallas import tpu as pltpu
from jax.sharding import PartitionSpec as P

NORM_EPS = 1e-6
MTP_WEIGHT = 0.3
F32 = jnp.float32
BF16 = jnp.bfloat16
I32 = jnp.int32
MESH = pl.DeviceIdType.MESH
VMEM_BYTES = 60 * 1024 * 1024
LANES = 128
GROUP = 16

ROWS_A = 288
FFN_TILE = 1024
HEAD_HALF = 1024
HEAD_PARTS = 4
CAP = 160
SLOTS = 4
BLOCK = 8


def rms(x_f):
    return x_f * lax.rsqrt(jnp.mean(x_f * x_f, axis=-1, keepdims=True) + NORM_EPS)


def rms_gain(x_val, gain_ref):
    return (rms(x_val.astype(F32)) * gain_ref[...].astype(F32)).astype(BF16)


def dot32(a, b):
    return jnp.dot(a, b, preferred_element_type=F32)


def norm_rows(dst, src, gain_ref=None, base=0):
    for r in range(0, src.shape[0], GROUP):
        val = rms(src[r:r + GROUP, :].astype(F32))
        if gain_ref is not None:
            val = val * gain_ref[...].astype(F32)
        dst[base + r:base + r + GROUP, :] = val.astype(BF16)


def collective(idx):
    return pltpu.CompilerParams(collective_id=idx, has_side_effects=True, vmem_limit_bytes=VMEM_BYTES)


def enter(peers):
    barrier = pltpu.get_barrier_semaphore()
    for peer in peers:
        pl.semaphore_signal(barrier, inc=1, device_id=peer, device_id_type=MESH)
    pl.semaphore_wait(barrier, len(peers))


def push(src, dst, send_sem, recv_sem, peer):
    return pltpu.make_async_remote_copy(
        src_ref=src, dst_ref=dst, send_sem=send_sem, recv_sem=recv_sem, device_id=peer, device_id_type=MESH
    )


def slot_ranks(held):
    row = lax.broadcasted_iota(I32, (LANES, LANES), 0)
    col = lax.broadcasted_iota(I32, (LANES, LANES), 1)
    ahead = dot32(held.astype(BF16), (row < col).astype(BF16))
    total = dot32(held.astype(BF16), jnp.ones((LANES, LANES), BF16))
    out, base = [], jnp.zeros((1, LANES), F32)
    for r in range(held.shape[0]):
        out.append(ahead[r:r + 1, :] + base)
        base = base + total[r:r + 1, :]
    return jnp.concatenate(out, axis=0)


def slots_kernel(n_data, n_local, ids_ref, idx_ref, most_ref, all_ref, got, send_sem, recv_sem):
    me, stage = lax.axis_index("dp"), lax.axis_index("pp")
    peers = [(jnp.bitwise_xor(me, k), stage) for k in range(1, n_data)]
    enter(peers)
    copies = [push(ids_ref, got.at[k], send_sem.at[k], recv_sem.at[k], peer) for k, peer in enumerate(peers)]
    for copy in copies:
        copy.start()
    for copy in copies:
        copy.wait()
    most = jnp.zeros((1, 1), F32)
    slot = lax.broadcasted_iota(I32, (CAP, LANES), 0).astype(F32)
    for k in range(n_data):
        ids = ids_ref[...] if k == 0 else got[k - 1]
        all_ref[k] = ids
        for s in range(n_data):
            inside = ((ids >= s * n_local) & (ids < (s + 1) * n_local)).astype(F32)
            most = jnp.maximum(most, jnp.sum(jnp.sum(inside, axis=1, keepdims=True), axis=0, keepdims=True))
        local = ids - me * n_local
        held = ((local >= 0) & (local < n_local)).astype(F32)
        rank = jnp.where(held > 0, slot_ranks(held), -1.0)
        high = lax.shift_right_arithmetic(local, 8)
        low = (local - high * 256).astype(F32)
        high = high.astype(F32)
        acc = jnp.zeros((BLOCK, CAP), F32)
        for r in range(ids.shape[0]):
            hit = (jnp.broadcast_to(rank[r:r + 1, :], (CAP, LANES)) == slot).astype(BF16)
            keep = held[r:r + 1, :]
            pair = jnp.concatenate(
                [high[r:r + 1, :] * keep, low[r:r + 1, :] * keep, jnp.zeros((BLOCK - 2, LANES), F32)], axis=0
            ).astype(BF16)
            acc = acc + lax.dot_general(pair, hit, (((1,), (1,)), ((), ())), preferred_element_type=F32)
        idx_ref[k:k + 1, :CAP] = (acc[0:1, :] * 256.0 + acc[1:2, :]).astype(I32)
    most_ref[...] = jnp.broadcast_to(most, most_ref.shape).astype(I32)


def run_slots(ids_tile, n_data, n_local):
    vmem = pl.BlockSpec(memory_space=pltpu.VMEM)
    return pl.pallas_call(
        functools.partial(slots_kernel, n_data, n_local),
        out_shape=[jax.ShapeDtypeStruct((n_data, 2 * LANES), I32), jax.ShapeDtypeStruct((BLOCK, LANES), I32),
                   jax.ShapeDtypeStruct((n_data, BLOCK, LANES), I32)],
        in_specs=[vmem],
        out_specs=[vmem, vmem, vmem],
        scratch_shapes=[
            pltpu.VMEM((n_data - 1, BLOCK, LANES), I32),
            pltpu.SemaphoreType.DMA((n_data - 1,)),
            pltpu.SemaphoreType.DMA((n_data - 1,)),
        ],
        compiler_params=collective(0),
        name="slots",
    )(ids_tile)


def pack_kernel(n_data, idx_ref, lane_ref, table_ref, o_ref, held, sems):
    parts = [(0, LANES), (LANES, CAP - LANES)]

    @pl.when(lax.axis_index("pp") == 0)
    def _():
        for k in range(n_data):
            for p, (first, count) in enumerate(parts):
                def fetch(c, carry):
                    start = pl.multiple_of(lax.shift_right_logical(idx_ref[k, first + c], 3) * BLOCK, BLOCK)
                    to = pl.multiple_of((k * CAP + first + c) * BLOCK, BLOCK)
                    pltpu.make_async_copy(
                        table_ref.at[pl.ds(start, BLOCK), :], held.at[pl.ds(to, BLOCK), :], sems.at[k * 2 + p]
                    ).start()
                    return carry

                lax.fori_loop(0, count, fetch, 0, unroll=8)
        for k in range(n_data):
            for p, (first, count) in enumerate(parts):
                at = (k * CAP + first) * BLOCK
                span = count * BLOCK
                pltpu.make_async_copy(table_ref.at[pl.ds(0, span), :], held.at[pl.ds(at, span), :], sems.at[k * 2 + p]).wait()
                idx = jnp.broadcast_to(lane_ref[k:k + 1, p * LANES:(p + 1) * LANES].astype(F32), (LANES, LANES))
                idx = jnp.transpose(idx)[:count, :].astype(I32)
                low = jnp.bitwise_and(idx, BLOCK - 1)
                row = lax.broadcasted_iota(I32, (count, LANES), 0)
                lane = lax.broadcasted_iota(I32, (count, LANES), 1)
                picks = []
                for c in range(0, span, LANES):
                    at_row = c // BLOCK + lax.shift_right_logical(lane, 3)
                    picks.append(((row == at_row) & (low == jnp.bitwise_and(lane, BLOCK - 1))).astype(F32).astype(BF16))
                pick = jnp.concatenate(picks, axis=1)
                o_ref[k, first:first + count, :] = dot32(pick, held[at:at + span, :]).astype(BF16)


def run_pack(idx, table):
    n_data = idx.shape[0]
    width = table.shape[1]
    return pl.pallas_call(
        functools.partial(pack_kernel, n_data),
        out_shape=jax.ShapeDtypeStruct((n_data, CAP, width), BF16),
        in_specs=[
            pl.BlockSpec(memory_space=pltpu.SMEM),
            pl.BlockSpec(memory_space=pltpu.VMEM),
            pl.BlockSpec(memory_space=pl.ANY),
        ],
        out_specs=pl.BlockSpec(memory_space=pltpu.VMEM),
        scratch_shapes=[pltpu.VMEM((n_data * CAP * BLOCK, width), BF16), pltpu.SemaphoreType.DMA((2 * n_data,))],
        compiler_params=pltpu.CompilerParams(vmem_limit_bytes=VMEM_BYTES),
        name="pack",
    )(idx, idx, table)


def trade_kernel(n_data, n_local, n_seq, ids_ref, packed_ref, x_ref, e_ref, got, pick_s, send_sem, recv_sem):
    me, stage = lax.axis_index("dp"), lax.axis_index("pp")
    n_tok = n_seq * LANES
    if x_ref.shape[0] > n_tok:
        x_ref[n_tok:, :] = jnp.zeros((x_ref.shape[0] - n_tok, x_ref.shape[1]), BF16)

    @pl.when(stage == 0)
    def _():
        peers = [(jnp.bitwise_xor(me, k), stage) for k in range(1, n_data)]
        enter(peers)
        copies = [
            push(packed_ref.at[k + 1], got.at[k], send_sem.at[k], recv_sem.at[k], peer) for k, peer in enumerate(peers)
        ]
        for k in (2, 0, 1):
            copies[k].start()
        ids = ids_ref[...]
        slot = lax.broadcasted_iota(I32, (CAP, LANES), 0).astype(F32)
        lane = lax.broadcasted_iota(I32, (1, LANES), 1)
        for k in range(n_data):
            src = jnp.bitwise_xor(me, k)
            held = ((ids >= src * n_local) & (ids < (src + 1) * n_local)).astype(F32)
            rank = jnp.where(held > 0, slot_ranks(held), -1.0)
            ahead = pltpu.roll(rank, LANES - 1, 1)
            for s in range(n_seq):
                now = rank[2 * s:2 * s + 1, :]
                later = jnp.where(lane == LANES - 1, ahead[2 * s + 1:2 * s + 2, :], ahead[2 * s:2 * s + 1, :])
                for q, want in ((s, now), (n_seq + s, later)):
                    hit = (jnp.broadcast_to(want, (CAP, LANES)) == slot).astype(F32).astype(BF16)
                    pick_s[k * CAP:(k + 1) * CAP, q * LANES:(q + 1) * LANES] = hit

        def placed(k, block):
            return lax.dot_general(
                pick_s[k * CAP:(k + 1) * CAP, :], block, (((0,), (0,)), ((), ())), preferred_element_type=F32
            ).astype(BF16)

        def add(val):
            x_ref[:n_tok, :] += val[:n_tok]
            e_ref[:n_tok, :] += val[n_tok:]

        first = placed(0, packed_ref[0])
        x_ref[:n_tok, :] = first[:n_tok]
        e_ref[:n_tok, :] = first[n_tok:]
        for k in (2, 0, 1):
            copies[k].wait()
            add(placed(k + 1, got[k]))

    @pl.when(stage != 0)
    def _():
        x_ref[:n_tok, :] = jnp.zeros((n_tok, x_ref.shape[1]), BF16)
        e_ref[:n_tok, :] = jnp.zeros((n_tok, x_ref.shape[1]), BF16)


def run_trade(ids_tile, packed, n_local, n_seq, pad_rows):
    n_data, _, width = packed.shape
    n_tok = n_seq * LANES
    vmem = pl.BlockSpec(memory_space=pltpu.VMEM)
    return pl.pallas_call(
        functools.partial(trade_kernel, n_data, n_local, n_seq),
        out_shape=[jax.ShapeDtypeStruct((pad_rows, width), BF16), jax.ShapeDtypeStruct((n_tok, width), BF16)],
        in_specs=[vmem, vmem],
        out_specs=[vmem, vmem],
        scratch_shapes=[
            pltpu.VMEM((n_data - 1, CAP, width), BF16),
            pltpu.VMEM((n_data * CAP, 2 * n_tok), BF16),
            pltpu.SemaphoreType.DMA((n_data - 1,)),
            pltpu.SemaphoreType.DMA((n_data - 1,)),
        ],
        compiler_params=collective(1),
        name="trade",
    )(ids_tile, packed)


def hand_on_kernel(rows_a, x_ref, e_ref, x_out, e_out, send_sem, recv_sem):
    me, stage = lax.axis_index("dp"), lax.axis_index("pp")
    peer = (me, 1 - stage)
    enter([peer])
    copies = [
        push(x_ref, x_out, send_sem.at[0], recv_sem.at[0], peer),
        push(e_ref.at[pl.ds(rows_a, e_out.shape[0]), :], e_out, send_sem.at[1], recv_sem.at[1], peer),
    ]

    @pl.when(stage == 0)
    def _():
        for copy in copies:
            copy.start()
        for copy in copies:
            copy.wait_send()

    @pl.when(stage != 0)
    def _():
        for copy in copies:
            copy.wait_recv()


def run_hand_on(x_val, e_val):
    rows_a, width = x_val.shape
    rows_b = e_val.shape[0] - rows_a
    hbm = pl.BlockSpec(memory_space=pl.ANY)
    return pl.pallas_call(
        functools.partial(hand_on_kernel, rows_a),
        out_shape=[jax.ShapeDtypeStruct((rows_a, width), BF16), jax.ShapeDtypeStruct((rows_b, width), BF16)],
        in_specs=[hbm, hbm],
        out_specs=[hbm, hbm],
        scratch_shapes=[pltpu.SemaphoreType.DMA((2,)), pltpu.SemaphoreType.DMA((2,))],
        compiler_params=collective(2),
        name="hand_on",
    )(x_val, e_val)


def swap_kernel(x_ref, o_ref, send_sem, recv_sem):
    peer = (lax.axis_index("dp"), 1 - lax.axis_index("pp"))
    enter([peer])
    copy = push(x_ref, o_ref, send_sem, recv_sem, peer)
    copy.start()
    copy.wait()


def run_swap(x_val):
    hbm = pl.BlockSpec(memory_space=pl.ANY)
    return pl.pallas_call(
        swap_kernel,
        out_shape=jax.ShapeDtypeStruct(x_val.shape, BF16),
        in_specs=[hbm],
        out_specs=hbm,
        scratch_shapes=[pltpu.SemaphoreType.DMA, pltpu.SemaphoreType.DMA],
        compiler_params=collective(3),
        name="swap",
    )(x_val)


def finish_kernel(n_data, n_stages, scale, x_ref, nll_ref, total_ref, got, send_sem, recv_sem):
    me, stage = lax.axis_index("dp"), lax.axis_index("pp")
    mine = me * n_stages + stage
    steps = [(k, c) for k in range(n_data) for c in range(n_stages) if (k, c) != (0, 0)]
    peers = [(jnp.bitwise_xor(me, k), jnp.bitwise_xor(stage, c)) for k, c in steps]
    enter(peers)
    copies = [push(x_ref, got.at[mine], send_sem.at[i], recv_sem.at[i], peer) for i, peer in enumerate(peers)]
    for copy in copies:
        copy.start()
    for copy in copies:
        copy.wait()
    got[mine] = x_ref[...]
    half = x_ref.shape[0] // 2
    total = jnp.zeros(x_ref.shape, F32)
    for i in range(n_data * n_stages):
        total = total + got[i]
    main = jnp.sum(jnp.sum(total[:half], axis=1, keepdims=True), axis=0, keepdims=True)
    mtp = jnp.sum(jnp.sum(total[half:], axis=1, keepdims=True), axis=0, keepdims=True)
    total_ref[...] = jnp.broadcast_to((main + MTP_WEIGHT * mtp) * scale, total_ref.shape)
    nll = x_ref[...]
    for c in range(1, n_stages):
        nll = nll + got[me * n_stages + jnp.bitwise_xor(stage, c)]
    nll_ref[...] = nll


def run_finish(tile, n_data, n_stages, scale):
    vmem = pl.BlockSpec(memory_space=pltpu.VMEM)
    n_peers = n_data * n_stages - 1
    return pl.pallas_call(
        functools.partial(finish_kernel, n_data, n_stages, scale),
        out_shape=[jax.ShapeDtypeStruct(tile.shape, F32), jax.ShapeDtypeStruct(tile.shape, F32)],
        in_specs=[vmem],
        out_specs=[vmem, vmem],
        scratch_shapes=[
            pltpu.VMEM((n_data * n_stages,) + tile.shape, F32),
            pltpu.SemaphoreType.DMA((n_peers,)),
            pltpu.SemaphoreType.DMA((n_peers,)),
        ],
        compiler_params=collective(4),
        name="finish",
    )(tile)


def ring_copy(src, ring, sems, i):
    slot = lax.rem(i, SLOTS)
    return pltpu.make_async_copy(src, ring.at[slot], sems.at[slot])


def ffn_steps(j, n_tiles, n_s, ready1, ready2, ring1, ring2, first, raw, hid, acc, finish):
    def slot1(t):
        return ring1[lax.rem(first[0] + t, SLOTS)]

    def slot2(t):
        return ring2[lax.rem(first[1] + t, SLOTS)]

    def activate():
        for r in range(0, raw.shape[0], GROUP):
            for c in range(0, raw.shape[1], 2 * LANES):
                spot = (slice(r, r + GROUP), slice(c, c + 2 * LANES))
                hid[spot] = jax.nn.gelu(raw[spot]).astype(BF16)

    @pl.when(j == 0)
    def _():
        ready1(0)
        raw[...] = dot32(n_s[...], slot1(0))

    @pl.when(j == 0)
    def _():
        ready1(1)
        ready2(0)
        activate()
        raw[...] = dot32(n_s[...], slot1(1))
        acc[...] = dot32(hid[...], slot2(0))

    @pl.when((j > 0) & (2 * j < n_tiles))
    def _():
        ready1(2 * j)
        ready1(2 * j + 1)
        ready2(2 * j - 1)
        ready2(2 * j)
        activate()
        raw[...] = dot32(n_s[...], slot1(2 * j))
        acc[...] += dot32(hid[...], slot2(2 * j - 1))
        activate()
        raw[...] = dot32(n_s[...], slot1(2 * j + 1))
        acc[...] += dot32(hid[...], slot2(2 * j))

    @pl.when(2 * j == n_tiles)
    def _():
        ready2(n_tiles - 1)
        activate()
        acc[...] += dot32(hid[...], slot2(n_tiles - 1))
        finish()


def layers_kernel(last_only, *refs):
    stage = lax.axis_index("pp")
    if last_only:
        @pl.when(stage != 0)
        def _():
            layers_body(*refs)
    else:
        layers_body(*refs)


def layers_body(own_ref, got_ref, w1_hbm, w2_hbm, o_ref, x_s, n_s, raw, hid, acc, ring1, ring2, sem1, sem2):
    layer, j = pl.program_id(0), pl.program_id(1)
    stage = lax.axis_index("pp")
    n_layers = w1_hbm.shape[1]
    n_tiles = w1_hbm.shape[3] // FFN_TILE
    total = n_layers * n_tiles
    first = layer * n_tiles

    def copy1(i):
        col = pl.multiple_of(lax.rem(i, n_tiles) * FFN_TILE, FFN_TILE)
        return ring_copy(w1_hbm.at[0, lax.div(i, n_tiles), :, pl.ds(col, FFN_TILE)], ring1, sem1, i)

    def copy2(i):
        row = pl.multiple_of(lax.rem(i, n_tiles) * FFN_TILE, FFN_TILE)
        return ring_copy(w2_hbm.at[0, lax.div(i, n_tiles), pl.ds(row, FFN_TILE), :], ring2, sem2, i)

    start = (layer == 0) & (j == 0)

    @pl.when(start)
    def _():
        copy1(0).start()

    @pl.when(start & (stage == 0))
    def _():
        x_s[...] = own_ref[...]

    @pl.when(start & (stage != 0))
    def _():
        x_s[...] = got_ref[...]

    @pl.when(j == 0)
    def _():
        norm_rows(n_s, x_s)

    @pl.when(start)
    def _():
        copy1(1).start()
        copy2(0).start()

    def feed(copy, i):
        @pl.when((2 * j < n_tiles) & (i < total))
        def _():
            copy(i).start()

    def ready1(t):
        copy1(first + t).wait()

    def ready2(t):
        copy2(first + t).wait()

    @pl.when(jnp.logical_not(start))
    def _():
        feed(copy1, first + 2 * j + 2)
        feed(copy2, first + 2 * j + 1)
        feed(copy1, first + 2 * j + 3)
        feed(copy2, first + 2 * j + 2)

    @pl.when(start)
    def _():
        copy1(0).wait()
        for i in (2, 3):
            copy1(i).start()
            copy2(i - 1).start()

    def ready1_once(t):
        if isinstance(t, int) and t == 0:
            @pl.when(layer > 0)
            def _():
                ready1(0)
        else:
            ready1(t)

    def finish():
        for r in range(0, x_s.shape[0], GROUP):
            rs = slice(r, r + GROUP)
            out = (x_s[rs, :].astype(F32) + acc[rs, :]).astype(BF16)
            x_s[rs, :] = out
            o_ref[rs, :] = out

    ffn_steps(j, n_tiles, n_s, ready1_once, ready2, ring1, ring2, (first, first), raw, hid, acc, finish)


def ring_scratch(width):
    return [
        pltpu.VMEM((SLOTS, width, FFN_TILE), BF16),
        pltpu.VMEM((SLOTS, FFN_TILE, width), BF16),
        pltpu.SemaphoreType.DMA((SLOTS,)),
        pltpu.SemaphoreType.DMA((SLOTS,)),
    ]


def run_layers(own, own_block, got, rows, w_one, w_two, last_only=False):
    width = own.shape[1]
    _, n_layers, _, ffn = w_one.shape
    n_tiles = ffn // FFN_TILE
    whole = pl.BlockSpec((rows, width), lambda l, j: (0, 0))
    hbm = pl.BlockSpec(memory_space=pl.ANY)
    return pl.pallas_call(
        functools.partial(layers_kernel, last_only),
        out_shape=jax.ShapeDtypeStruct((rows, width), BF16),
        grid=(n_layers, n_tiles // 2 + 1),
        in_specs=[pl.BlockSpec((rows, width), lambda l, j: (own_block, 0)), whole, hbm, hbm],
        out_specs=whole,
        scratch_shapes=[
            pltpu.VMEM((rows, width), BF16),
            pltpu.VMEM((rows, width), BF16),
            pltpu.VMEM((rows, FFN_TILE), F32),
            pltpu.VMEM((rows, FFN_TILE), BF16),
            pltpu.VMEM((rows, width), F32),
        ] + ring_scratch(width),
        compiler_params=pltpu.CompilerParams(dimension_semantics=("arbitrary", "arbitrary"), vmem_limit_bytes=VMEM_BYTES),
        cost_estimate=pl.CostEstimate(
            flops=4 * rows * width * ffn * n_layers, bytes_accessed=4 * width * ffn * n_layers, transcendentals=0
        ),
        name="layers",
    )(own, got, w_one, w_two)


def mtp_kernel(
    n_proj, n_tiles, own_h, own_e, got_h, got_e, gain_ref, wp_hbm, w1_hbm, w2_hbm, o_ref,
    cat_s, z_s, n_s, raw, hid, acc, ring1, ring2, sem1, sem2,
):
    step = pl.program_id(0)
    stage = lax.axis_index("pp")
    rows, width = own_h.shape
    rows_b = got_h.shape[0]
    proj_steps = n_proj // 2
    j = step - proj_steps
    gf_ref, gh_ref, ge_ref, gm_ref = (gain_ref.at[k:k + 1, :] for k in range(4))

    def copy1(i):
        col = pl.multiple_of(i * FFN_TILE, FFN_TILE)
        return ring_copy(w1_hbm.at[:, pl.ds(col, FFN_TILE)], ring1, sem1, i)

    def copy2(i):
        row = pl.multiple_of((i - n_proj) * FFN_TILE, FFN_TILE)
        return ring_copy(w2_hbm.at[pl.ds(row, FFN_TILE), :], ring2, sem2, i)

    def copyp(i):
        return ring_copy(wp_hbm.at[pl.ds(i * FFN_TILE, FFN_TILE), :], ring2, sem2, i)

    @pl.when(step == 0)
    def _():
        copyp(0).start()
        copyp(1).start()

    @pl.when((step == 0) & (stage == 0))
    def _():
        z_s[...] = own_h[...]
        n_s[...] = own_e[...]

    @pl.when((step == 0) & (stage != 0))
    def _():
        z_s[:rows_b, :] = got_h[...]
        n_s[:rows_b, :] = got_e[...]
        if rows_b < rows:
            z_s[rows_b:, :] = jnp.zeros((rows - rows_b, width), BF16)
            n_s[rows_b:, :] = jnp.zeros((rows - rows_b, width), BF16)

    @pl.when(step == 0)
    def _():
        norm_rows(cat_s.at[:, pl.ds(0, width)], z_s, gh_ref)
        norm_rows(cat_s.at[:, pl.ds(width, width)], n_s, ge_ref)
        norm_rows(o_ref, z_s, gf_ref)
        acc[...] = jnp.zeros_like(acc)
        copyp(2).start()
        copyp(3).start()

    for p in range(proj_steps):
        @pl.when(step == p)
        def _():
            for t in (2 * p, 2 * p + 1):
                copyp(t).wait()
            if p == proj_steps - 1:
                copy1(0).start()
                copy1(1).start()
                copy2(n_proj).start()

    @pl.when(step < proj_steps)
    def _():
        for half in range(2):
            at = pl.multiple_of((2 * step + half) * FFN_TILE, FFN_TILE)
            acc[...] += dot32(cat_s[:, pl.ds(at, FFN_TILE)], ring2[lax.rem(2 * step + half, SLOTS)])

    @pl.when(step == proj_steps - 1)
    def _():
        for r in range(0, rows, GROUP):
            z_s[r:r + GROUP, :] = acc[r:r + GROUP, :].astype(BF16)
        norm_rows(n_s, z_s, gm_ref)

    def feed(copy, i, end):
        @pl.when((j >= 0) & (2 * j < n_tiles) & (i < end))
        def _():
            copy(i).start()

    feed(copy1, 2 * j + 2, n_tiles)
    feed(copy2, n_proj + 2 * j + 1, n_proj + n_tiles)
    feed(copy1, 2 * j + 3, n_tiles)
    feed(copy2, n_proj + 2 * j + 2, n_proj + n_tiles)

    def ready1(t):
        copy1(t).wait()

    def ready2(t):
        copy2(n_proj + t).wait()

    def finish():
        for r in range(0, rows, GROUP):
            rs = slice(r, r + GROUP)
            z_s[rs, :] = (z_s[rs, :].astype(F32) + acc[rs, :]).astype(BF16)

    ffn_steps(j, n_tiles, n_s, ready1, ready2, ring1, ring2, (0, n_proj), raw, hid, acc, finish)

    @pl.when((2 * j == n_tiles) & (stage == 0))
    def _():
        norm_rows(o_ref, z_s, gf_ref, rows)

    @pl.when((2 * j == n_tiles) & (stage != 0))
    def _():
        norm_rows(o_ref, z_s.at[pl.ds(0, rows_b), :], gf_ref, rows_b)


def run_mtp(own_h, own_e, got_h, got_e, gains, w_proj, u_one, u_two):
    rows, width = own_h.shape
    rows_b = got_h.shape[0]
    ffn = u_one.shape[1]
    n_tiles = ffn // FFN_TILE
    n_proj = w_proj.shape[0] // FFN_TILE
    assert n_proj == SLOTS
    whole = pl.BlockSpec((rows, width), lambda s: (0, 0))
    other = pl.BlockSpec((rows_b, width), lambda s: (0, 0))
    hbm = pl.BlockSpec(memory_space=pl.ANY)
    return pl.pallas_call(
        functools.partial(mtp_kernel, n_proj, n_tiles),
        out_shape=jax.ShapeDtypeStruct((2 * rows, width), BF16),
        grid=(n_proj // 2 + n_tiles // 2 + 1,),
        in_specs=[whole, whole, other, other, pl.BlockSpec(gains.shape, lambda s: (0, 0)), hbm, hbm, hbm],
        out_specs=pl.BlockSpec((2 * rows, width), lambda s: (0, 0)),
        scratch_shapes=[
            pltpu.VMEM((rows, 2 * width), BF16),
            pltpu.VMEM((rows, width), BF16),
            pltpu.VMEM((rows, width), BF16),
            pltpu.VMEM((rows, FFN_TILE), F32),
            pltpu.VMEM((rows, FFN_TILE), BF16),
            pltpu.VMEM((rows, width), F32),
        ] + ring_scratch(width),
        compiler_params=pltpu.CompilerParams(dimension_semantics=("arbitrary",), vmem_limit_bytes=VMEM_BYTES),
        cost_estimate=pl.CostEstimate(
            flops=4 * rows * width * (ffn + width), bytes_accessed=4 * width * (ffn + width), transcendentals=0
        ),
        name="mtp",
    )(own_h, own_e, got_h, got_e, gains, w_proj, u_one, u_two)


def head_stats(rows, buf, n_cols, base, tgt_ref, m_ref, s_ref, p_ref):
    lane = lax.broadcasted_iota(jnp.int32, (GROUP, LANES), 1)
    for r in range(0, rows, GROUP):
        rs = slice(r, r + GROUP)
        parts = [buf[rs, c:c + LANES] for c in range(0, n_cols, LANES)]
        top = parts[0]
        for part in parts[1:]:
            top = jnp.maximum(top, part)
        m_old = m_ref[rs, :]
        m_new = jnp.maximum(m_old, top)
        total = s_ref[rs, :] * jnp.exp(m_old - m_new)
        rel = tgt_ref[rs, :] - lane - base
        pick = p_ref[rs, :]
        for k, part in enumerate(parts):
            total = total + jnp.exp(part - m_new)
            pick = jnp.where(rel == k * LANES, part, pick)
        m_ref[rs, :] = m_new
        s_ref[rs, :] = total
        p_ref[rs, :] = pick


def head_kernel(n_steps, tail, parts, x_ref, tgt_ref, w_ref, o_ref, buf_a, buf_b, t_ref, m_ref, s_ref, p_ref):
    stage = lax.axis_index("pp")
    for s, (first, count) in enumerate(parts):
        @pl.when(stage == s)
        def _():
            head_body(n_steps, tail, first, count, x_ref, tgt_ref, w_ref, o_ref, buf_a, buf_b, t_ref, m_ref, s_ref, p_ref)


def head_body(n_steps, tail, first, count, x_ref, tgt_ref, w_ref, o_ref, buf_a, buf_b, t_ref, m_ref, s_ref, p_ref):
    i = pl.program_id(0)
    half = buf_a.shape[1]
    rows = 2 * count
    n_seq = tgt_ref.shape[0] // 2
    bufs = (buf_a, buf_b)
    state = (t_ref, m_ref, s_ref, p_ref)
    row = lax.broadcasted_iota(I32, (GROUP, LANES), 0)
    lane = lax.broadcasted_iota(I32, (GROUP, LANES), 1)

    @pl.when(i == 0)
    def _():
        m_ref[...] = jnp.full_like(m_ref, -3e38)
        s_ref[...] = jnp.zeros_like(s_ref)
        p_ref[...] = jnp.zeros_like(p_ref)
        for part in range(2):
            for r in range(0, count, GROUP):
                want = jnp.zeros((GROUP, LANES), F32)
                for q in range(n_seq):
                    line = tgt_ref[part * n_seq + q:part * n_seq + q + 1, :].astype(F32)
                    want = want + jnp.where(q * LANES + lane == first + r + row, jnp.broadcast_to(line, want.shape), 0.0)
                want = jnp.sum(want, axis=1, keepdims=True)
                at = part * count + r
                t_ref[at:at + GROUP, :] = jnp.broadcast_to(want, (GROUP, LANES)).astype(I32)
        base = (n_steps - 1) * HEAD_PARTS * half
        for k, done in enumerate(range(0, tail, half)):
            cols = min(half, tail - done)
            bufs[k % 2][:rows, :cols] = dot32(x_ref[:rows, :], w_ref[:, done:done + cols])
            head_stats(rows, bufs[k % 2], cols, base + done, *state)
        buf_b[...] = jnp.full_like(buf_b, -3e38)

    @pl.when(i > 0)
    def _():
        base = (i - 1) * HEAD_PARTS * half
        for q in range(HEAD_PARTS):
            bufs[q % 2][:rows, :] = dot32(x_ref[:rows, :], w_ref[:, q * half:(q + 1) * half])
            head_stats(rows, bufs[(q + 1) % 2], half, base + (q - 1) * half, *state)

    @pl.when(i == n_steps - 1)
    def _():
        head_stats(rows, buf_b, half, (i * HEAD_PARTS - 1) * half, *state)
        for part in range(2):
            lines = [jnp.zeros((1, LANES), F32) for _ in range(n_seq)]
            for r in range(0, count, GROUP):
                rs = slice(part * count + r, part * count + r + GROUP)
                top = jnp.max(m_ref[rs, :], axis=1, keepdims=True)
                total = jnp.sum(s_ref[rs, :] * jnp.exp(m_ref[rs, :] - top), axis=1, keepdims=True)
                picked = jnp.sum(p_ref[rs, :], axis=1, keepdims=True)
                nll = jnp.broadcast_to(top + jnp.log(total) - picked, (GROUP, LANES))
                for q in range(n_seq):
                    if q * LANES < first + r + GROUP and first + r < (q + 1) * LANES:
                        here = jnp.where(q * LANES + lane == first + r + row, nll, 0.0)
                        lines[q] = lines[q] + jnp.sum(here, axis=0, keepdims=True)
            o_ref[part * n_seq:(part + 1) * n_seq, :] = jnp.concatenate(lines, axis=0)


def run_head(x_val, tgt_tile, parts, w_out):
    rows, width = x_val.shape
    vocab = w_out.shape[1]
    tile = HEAD_PARTS * HEAD_HALF
    n_steps = pl.cdiv(vocab, tile)
    tail = vocab - (n_steps - 1) * tile
    small = pl.BlockSpec(tgt_tile.shape, lambda i: (0, 0))
    return pl.pallas_call(
        functools.partial(head_kernel, n_steps, tail, parts),
        out_shape=jax.ShapeDtypeStruct(tgt_tile.shape, F32),
        grid=(n_steps,),
        in_specs=[
            pl.BlockSpec((rows, width), lambda i: (0, 0)),
            small,
            pl.BlockSpec((width, tile), lambda i: (0, jnp.where(i == 0, n_steps - 1, i - 1))),
        ],
        out_specs=small,
        scratch_shapes=[pltpu.VMEM((rows, HEAD_HALF), F32)] * 2
        + [pltpu.VMEM((rows, LANES), I32)]
        + [pltpu.VMEM((rows, LANES), F32)] * 3,
        compiler_params=pltpu.CompilerParams(dimension_semantics=("arbitrary",), vmem_limit_bytes=VMEM_BYTES),
        cost_estimate=pl.CostEstimate(flops=2 * rows * width * vocab, bytes_accessed=2 * width * vocab, transcendentals=0),
        name="head",
    )(x_val, tgt_tile, w_out)


def solution(mesh):
    n_data = mesh.shape["dp"]
    n_stages = mesh.shape["pp"]

    def swap_perm(k):
        return [(d * n_stages, (d ^ k) * n_stages) for d in range(n_data)]

    def extra_rows(table, ids_all, j):
        me = lax.axis_index("dp")
        n_local = table.shape[0]
        ids_all = jnp.where(j > 0, ids_all, 0)
        n = ids_all.shape[1]
        before = (jnp.arange(n)[:, None] < jnp.arange(n)[None, :]).astype(BF16)
        owner = ids_all // n_local

        def ranks(held):
            return dot32(held.astype(BF16), before).astype(I32) - j * CAP

        held = owner == me
        hit = held[:, None, :] & (ranks(held)[:, None, :] == jnp.arange(CAP)[None, :, None])
        idx = jnp.sum(jnp.where(hit, (ids_all - me * n_local)[:, None, :], 0), axis=2)
        got = [table[idx[0]]] + [lax.ppermute(table[idx[k]], ("dp", "pp"), swap_perm(k)) for k in range(1, n_data)]
        src = jnp.bitwise_xor(owner[0], me)
        mine = src[None, :] == jnp.arange(n_data)[:, None]
        rank = jnp.sum(jnp.where(mine, ranks(mine), 0), axis=0)
        place = jnp.where((rank >= 0) & (rank < CAP), src * CAP + rank, -1)
        pick = (place[:, None] == jnp.arange(n_data * CAP)[None, :]).astype(BF16)
        return dot32(pick, jnp.concatenate(got, axis=0)).astype(BF16)

    def body(tok_ids, emb_s, w_one, w_two, gain_f, gain_h, gain_e, gain_m, w_proj, u_one, u_two, w_out):
        n_micro, batch_dev, seq_plus = tok_ids.shape
        seq_len = seq_plus - 2
        n_seq = n_micro * batch_dev
        n_tok = n_seq * seq_len
        assert seq_len == LANES and 2 * n_seq == BLOCK
        rows_a = ROWS_A
        rows_b = n_tok - rows_a
        table = emb_s[0]
        n_local = table.shape[0]
        ids = tok_ids.reshape(n_seq, seq_plus)
        spare = jnp.full((n_seq, seq_len - 1), -1, I32)
        ids_tile = jnp.concatenate([ids[:, :seq_len + 1], spare], axis=1).reshape(2 * n_seq, seq_len)
        tgt_tile = jnp.concatenate([ids[:, 1:seq_len + 1], ids[:, 2:]], axis=0)

        idx, most, ids_seen = run_slots(ids_tile, n_data, n_local)
        packed = run_pack(idx, table)
        x_all, e_all = run_trade(ids_tile, packed, n_local, n_seq, 2 * rows_a)

        def more(carry):
            j, x_val, e_val = carry
            wanted = ids_seen.reshape(n_data, n_seq, 2 * seq_len)[:, :, :seq_len + 1].reshape(n_data, -1)
            rows = extra_rows(table, wanted, j).reshape(n_seq, seq_len + 1, -1)
            x_more = rows[:, :seq_len].reshape(n_tok, -1)
            e_more = rows[:, 1:].reshape(n_tok, -1)
            return j + 1, x_val + jnp.pad(x_more, ((0, 2 * rows_a - n_tok), (0, 0))), e_val + e_more

        most = most[0, 0]
        _, x_all, e_all = lax.while_loop(lambda c: c[0] * CAP < most, more, (jnp.int32(1), x_all, e_all))

        x_mid = run_layers(x_all, 0, x_all, rows_a, w_one, w_two)
        moved, e_last = run_hand_on(x_mid, e_all)
        swapped = run_swap(run_layers(x_all, 1, moved, rows_a, w_one, w_two))

        h_last = run_layers(swapped, 0, swapped, rows_b, w_one, w_two, last_only=True)
        gains = jnp.stack([gain_f, gain_h, gain_e, gain_m] * 2).astype(F32)
        normed = run_mtp(swapped, e_all, h_last, e_last, gains, w_proj, u_one, u_two)
        tile = run_head(normed, tgt_tile, ((0, rows_a), (rows_a, rows_b)), w_out)
        nll, total = run_finish(tile, n_data, n_stages, 1.0 / (n_tok * n_data))
        shape = (n_micro, batch_dev, seq_len)
        return total[0, 0], nll[:n_seq].reshape(shape), nll[n_seq:].reshape(shape)

    rep = P()
    in_specs = (P(None, "dp", None), P("pp", "dp", None), P("pp"), P("pp")) + (rep,) * 8
    out_specs = (rep, P(None, "dp", None), P(None, "dp", None))
    return jax.shard_map(body, mesh=mesh, in_specs=in_specs, out_specs=out_specs, check_vma=False)
```
